32 devices in a mesh: data: 1 (over z), tp: 32 (over y, x, core).
Axes of the slice: x: 4, y: 4, z: 1, core: 2. Of those that a mesh axis runs over, the one named last changes fastest.
The devices are a block of a 4x4x8 slice.
Arguments:
- X: bfloat16 [2048, 2048], P(('data', 'tp'))
- gamma: float32 [2048], replicated
- W1: bfloat16 [2048, 32768], P(None, 'tp')
- W2: bfloat16 [32768, 2048], P('tp')
- dY: bfloat16 [2048, 2048], P(('data', 'tp'))
Outputs:
- output 1: bfloat16 [2048, 2048], P(('data', 'tp'))
- output 2: bfloat16 [2048, 2048], P(('data', 'tp'))
- output 3: float32 [2048, 32768], P('data', 'tp')
- output 4: float32 [32768, 2048], P(('data', 'tp'))
- output 5: float32 [2048], P('data')
All inputs are finite; a program needn't handle non-finite values.
Results may differ from the reference program's by a relative error of at most 0.00102.
Values are sent between devices in bfloat16 or wider.
A program may use at most 768 MiB of HBM per device.

```python
import jax
import jax.numpy as jnp
from jax import lax

S = 2048
D = 2048
F = 32768
EPS = 1e-6


def setup_inputs(seed: int = 0, part: int = 0) -> dict:
    key = jax.random.key(seed)
    kg, k1, k2, kbase = jax.random.split(key, 4)
    kx, ky = jax.random.split(jax.random.fold_in(kbase, part))
    X = jax.random.normal(kx, (S, D), jnp.float32).astype(jnp.bfloat16)
    gamma = 1.0 + 0.2 * jax.random.normal(kg, (D,), jnp.float32)
    W1 = (jax.random.normal(k1, (D, F), jnp.float32) * D ** -0.5).astype(jnp.bfloat16)
    W2 = (jax.random.normal(k2, (F, D), jnp.float32) * (1.5 * F ** -0.5)).astype(jnp.bfloat16)
    dY = jax.random.normal(ky, (S, D), jnp.float32).astype(jnp.bfloat16)
    return {"X": X, "gamma": gamma, "W1": W1, "W2": W2, "dY": dY}


def _gelu(a):
    return jax.nn.gelu(a, approximate=True)


def reference(X, gamma, W1, W2, dY):
    x = X.astype(jnp.float32)
    mu = jnp.mean(x, axis=-1, keepdims=True)
    xc = x - mu
    var = jnp.mean(xc * xc, axis=-1, keepdims=True)
    rstd = lax.rsqrt(var + EPS)
    xhatv = xc * rstd
    Xn = (xhatv * gamma).astype(jnp.bfloat16)
    A = jnp.dot(Xn, W1, preferred_element_type=jnp.float32)
    H = _gelu(A).astype(jnp.bfloat16)
    Y = (x + jnp.dot(H, W2, preferred_element_type=jnp.float32)).astype(jnp.bfloat16)
    dW2 = jnp.dot(H.T, dY, preferred_element_type=jnp.float32)
    dH = jnp.dot(dY, W2.T, preferred_element_type=jnp.float32)
    dA = jax.vjp(_gelu, A)[1](dH)[0].astype(jnp.bfloat16)
    dW1 = jnp.dot(Xn.T, dA, preferred_element_type=jnp.float32)
    dXn = jnp.dot(dA, W1.T, preferred_element_type=jnp.float32)
    dgamma = jnp.sum(dXn * xhatv, axis=0)
    dxhat = dXn * gamma
    dx = rstd * (dxhat - jnp.mean(dxhat, axis=-1, keepdims=True) - xhatv * jnp.mean(dxhat * xhatv, axis=-1, keepdims=True))
    dX = (dY.astype(jnp.float32) + dx).astype(jnp.bfloat16)
    return (Y, dX, dW1, dW2, dgamma)
```

```python
import math

import jax
import jax.numpy as jnp
from jax import lax
from jax.sharding import PartitionSpec as P

EPS = 1e-6


def _gelu(a):
    return jax.nn.gelu(a, approximate=True)


def _ln(x):
    mu = jnp.mean(x, axis=-1, keepdims=True)
    xc = x - mu
    var = jnp.mean(xc * xc, axis=-1, keepdims=True)
    rstd = lax.rsqrt(var + EPS)
    return xc * rstd, rstd


def _nn(a, b):
    return jnp.dot(a, b, preferred_element_type=jnp.float32)


def _tn(a, b):
    return lax.dot_general(a, b, (((0,), (0,)), ((), ())), preferred_element_type=jnp.float32)


def _nt(a, b):
    return lax.dot_general(a, b, (((1,), (1,)), ((), ())), preferred_element_type=jnp.float32)


REL = (0, 1, -1, 2)


def _torus(n):
    side = math.isqrt(n // 2)
    assert side * side * 2 == n and side == 4

    def perm(dy, dx, dc):
        return [((y * side + x) * 2 + c, ((y + dy) % side * side + (x + dx) % side) * 2 + (c + dc) % 2)
                for y in range(side) for x in range(side) for c in range(2)]

    def mover(p):
        return lambda v: lax.ppermute(v, "tp", p)

    yplus, yminus = mover(perm(1, 0, 0)), mover(perm(-1, 0, 0))
    xplus, xminus = mover(perm(0, 1, 0)), mover(perm(0, -1, 0))
    return (yplus, yminus), (xplus, xminus), mover(perm(0, 0, 1)), mover(perm(2, 0, 0)), mover(perm(0, 2, 0))


def _ring_gather(b, ring):
    plus, minus = ring
    h = b.shape[0] // 2
    prev, nxt = plus(b), minus(b)
    far = jnp.concatenate([plus(prev[:h]), minus(nxt[h:])], axis=0)
    return {0: b, 1: nxt, -1: prev, 2: far}


def _ring_scatter(p1, p2, ring):
    plus, minus = ring
    f1 = plus(p1[2])
    f2 = minus(p2[2])
    d2 = plus(p2[1])
    d1 = minus(p1[-1])
    g1 = plus(p1[1] + f1)
    g2 = minus(p2[-1] + f2)
    return p1[0] + d1 + g1, p2[0] + d2 + g2


def solution(mesh):
    rows = P(("data", "tp"), None)
    yring, xring, swap, yfar, xfar = _torus(mesh.shape["tp"])

    def gather(b, first, second, key):
        line = _ring_gather(b, first)
        grid = {r: _ring_gather(line[r], second) for r in REL}
        out = {}
        for dy in REL:
            parts = [grid[dx][dy] if key == "x" else grid[dy][dx] for dx in REL]
            own = jnp.concatenate(parts, axis=0)
            out[dy] = (own, swap(own))
        return out

    def scatter(own, other):
        d = own[0].shape[1]
        q = d // 4
        r = own[0].shape[0] // 4
        got = {dy: swap(other[dy]) for dy in REL}

        def acc(dy, k, dx=None):
            sl = (slice(None) if dx is None else slice(REL.index(dx) * r, (REL.index(dx) + 1) * r), slice(k * q, (k + 1) * q))
            return own[dy][sl] + got[dy][sl]

        a1, a2 = _ring_scatter({dy: acc(dy, 0) for dy in REL}, {dy: acc(dy, 1) for dy in REL}, yring)
        part = lambda z: {dx: z[i * r:(i + 1) * r] for i, dx in enumerate(REL)}
        a1, a2 = _ring_scatter(part(a1), part(a2), xring)
        stack = lambda k: {dx: jnp.concatenate([acc(dy, k, dx) for dy in REL], axis=0) for dx in REL}
        b1, b2 = _ring_scatter(stack(2), stack(3), xring)
        b1, b2 = _ring_scatter(part(b1), part(b2), yring)
        return jnp.concatenate([a1, a2, b1, b2], axis=1)

    def allsum(v):
        v = v + swap(v)
        v = v + xring[0](v) + xring[1](v) + xfar(v)
        return v + yring[0](v) + yring[1](v) + yfar(v)

    def body(X, gamma, W1, W2, dY):
        x = X.astype(jnp.float32)
        xhatv, rstd = _ln(x)
        gs = gather(dY, yring, xring, "y")
        xs = gather((xhatv * gamma).astype(jnp.bfloat16), xring, yring, "x")
        Hs, As, gcat, xcat, yp, dxp = {}, {}, {}, {}, {}, {}
        half = X.shape[0] * 4
        for dy in REL:
            xcat[dy] = jnp.concatenate(xs[dy], axis=0)
            A = _nn(xcat[dy], W1)
            H = _gelu(A).astype(jnp.bfloat16)
            Hs[dy] = H
            As[dy] = A
            yp[dy] = (_nn(H[:half], W2), _nn(H[half:], W2))
        Y = (x + scatter({k: v[0] for k, v in yp.items()}, {k: v[1] for k, v in yp.items()})).astype(jnp.bfloat16)
        dAs = {}
        for dy in REL:
            gcat[dy] = jnp.concatenate(gs[dy], axis=0)
            dH = _nt(gcat[dy], W2)
            dA = jax.vjp(_gelu, As[dy])[1](dH)[0].astype(jnp.bfloat16)
            dAs[dy] = dA
            dxp[dy] = (_nt(dA[:half], W1), _nt(dA[half:], W1))
        dXn = scatter({k: v[0] for k, v in dxp.items()}, {k: v[1] for k, v in dxp.items()})
        cat = lambda t: jnp.concatenate([t[dy] for dy in REL], axis=0)
        dW2 = _tn(cat(Hs), cat(gcat))
        dW1 = _tn(cat(xcat), cat(dAs))
        dgamma = allsum(jnp.sum(dXn * xhatv, axis=0))
        dxhat = dXn * gamma
        dx = rstd * (dxhat - jnp.mean(dxhat, axis=-1, keepdims=True) - xhatv * jnp.mean(dxhat * xhatv, axis=-1, keepdims=True))
        dX = (dY.astype(jnp.float32) + dx).astype(jnp.bfloat16)
        return Y, dX, dW1, dW2, dgamma

    return jax.shard_map(body, mesh=mesh,
                         in_specs=(rows, P(None), P(None, "tp"), P("tp", None), rows),
                         out_specs=(rows, rows, P("data", "tp"), rows, P("data")),
                         check_vma=False)
```

```python
import math

import jax
import jax.numpy as jnp
from jax import lax
from jax.experimental import pallas as pl
from jax.experimental.pallas import tpu as pltpu
from jax.sharding import PartitionSpec as P

EPS = 1e-6
BF16 = jnp.bfloat16
F32 = jnp.float32
MESH = pl.DeviceIdType.MESH

REL = (0, 1, -1, 2)
IX = {0: 0, 1: 1, -1: 2, 2: 3}
ORDER = (0, 1, -1, 2)
SIDE = 4


def _dot(a, b, ca, cb):
    return lax.dot_general(a, b, (((ca,), (cb,)), ((), ())), preferred_element_type=F32)


def _ln(x):
    mu = jnp.mean(x, axis=-1, keepdims=True)
    xc = x - mu
    var = jnp.mean(xc * xc, axis=-1, keepdims=True)
    rstd = lax.rsqrt(var + EPS)
    return xc * rstd, rstd


def _gelu_and_grad(a):
    c = math.sqrt(2.0 / math.pi)
    a2 = a * a
    t = jnp.tanh(c * (a + 0.044715 * (a2 * a)))
    cdf = 0.5 * (1.0 + t)
    grad = cdf + (0.5 * a * (1.0 - t * t)) * (c + (3.0 * 0.044715 * c) * a2)
    return a * cdf, grad


def _kernel(x_ref, g_ref, w1_hbm, w2_hbm, dy_hbm,
            y_out, dx_out, dg_out, dw1_hbm, dw2_hbm,
            xn, dy, h, da, w1, w2, acc, zbuf, stage, sibr, r1, r2, ysum, gam, gin, dwst,
            ags, agr, p1s, p1r, p2s, p2r, sbs, sbr, gs, gr, lsem, c1, c2, csib):
    me = lax.axis_index("tp")
    core = me % 2
    cx = (me // 2) % SIDE
    cy = me // (2 * SIDE)

    def dev(yy, xx, cc):
        return {"tp": ((yy % SIDE) * SIDE + (xx % SIDE)) * 2 + cc}

    yp, ym, yf = dev(cy + 1, cx, core), dev(cy + SIDE - 1, cx, core), dev(cy + 2, cx, core)
    xp, xm, xf = dev(cy, cx + 1, core), dev(cy, cx + SIDE - 1, core), dev(cy, cx + 2, core)
    sib = dev(cy, cx, 1 - core)

    R = x_ref.shape[0]
    HR = R // 2
    D = x_ref.shape[1]
    FS = w1.shape[1]
    BLK = 2 * SIDE * R
    OWN = SIDE * R
    C = D // 2
    Q = C // 4

    cw1 = pltpu.make_async_copy(w1_hbm, w1, lsem.at[0])
    cw2 = pltpu.make_async_copy(w2_hbm, w2, lsem.at[1])
    cdy = pltpu.make_async_copy(dy_hbm, dy.at[pl.ds(0, R)], lsem.at[2])
    cdy.start()
    cw1.start()
    cw2.start()
    xhat, rstd = _ln(x_ref[...].astype(F32))
    xn[0:R, :] = (xhat * g_ref[...]).astype(BF16)

    bar = pltpu.get_barrier_semaphore()
    for d in (yp, ym, yf, xp, xm, xf, sib):
        pl.semaphore_signal(bar, inc=1, device_id=d, device_id_type=MESH)
    pl.semaphore_wait(bar, 7)

    def remote(src, dst, ss, rs, d):
        return pltpu.make_async_remote_copy(src_ref=src, dst_ref=dst, send_sem=ss, recv_sem=rs, device_id=d, device_id_type=MESH)

    pending = []

    def go(c):
        c.start()
        pending.append(c)

    class Gather:
        def __init__(self, buf, first, second, xfirst, base):
            n = [base]

            def at(r1_, r2_, half=None):
                dd, ee = (r2_, r1_) if xfirst else (r1_, r2_)
                o = (IX[dd] * 2 * SIDE + IX[ee]) * R
                if half is None:
                    return buf.at[pl.ds(o, R)]
                return buf.at[pl.ds(o + half * HR, HR)]

            def mk(src, dst, d):
                i = n[0]
                n[0] += 1
                return remote(src, dst, ags.at[i], agr.at[i], d)

            (fp, fm), (sp, sm) = first, second
            self.d1p = mk(at(0, 0), at(-1, 0), fp)
            self.d1m = mk(at(0, 0), at(1, 0), fm)
            self.d1hp = mk(at(-1, 0, 0), at(2, 0, 0), fp)
            self.d1hm = mk(at(1, 0, 1), at(2, 0, 1), fm)
            self.d2p = {r: mk(at(r, 0), at(r, -1), sp) for r in REL}
            self.d2m = {r: mk(at(r, 0), at(r, 1), sm) for r in REL}
            self.d2hp = {r: mk(at(r, -1, 0), at(r, 2, 0), sp) for r in REL}
            self.d2hm = {r: mk(at(r, 1, 1), at(r, 2, 1), sm) for r in REL}
            self.sb = {r: mk(buf.at[pl.ds(IX[r] * BLK, OWN)], buf.at[pl.ds(IX[r] * BLK + OWN, OWN)], sib) for r in REL}

    gx = Gather(xn, (xp, xm), (yp, ym), True, 0)
    gy = Gather(dy, (yp, ym), (xp, xm), False, 24)

    cdy.wait()
    for g in (gx, gy):
        go(g.d1p)
        go(g.d1m)
    for g in (gx, gy):
        go(g.d2p[0])
        go(g.d2m[0])
    for g in (gx, gy):
        g.d1p.wait_recv()
        go(g.d1hp)
        g.d1m.wait_recv()
        go(g.d1hm)
    for r in (1, -1):
        for g in (gx, gy):
            go(g.d2p[r])
            go(g.d2m[r])
    gy.d2p[0].wait_recv()
    go(gy.d2hp[0])
    gy.d2m[0].wait_recv()
    go(gy.d2hm[0])
    for g in (gx, gy):
        g.d1hp.wait_recv()
        g.d1hm.wait_recv()
        go(g.d2p[2])
        go(g.d2m[2])
    go(gx.sb[0])
    gy.d2hp[0].wait_recv()
    gy.d2hm[0].wait_recv()
    go(gy.sb[0])

    TF = 512

    def hidden(dd):
        o = IX[dd] * BLK

        def step(f, _):
            fo = pl.multiple_of(f * TF, TF)
            a = _dot(xn[o:o + BLK, :], w1[:, pl.ds(fo, TF)], 1, 0)
            dh = _dot(dy[o:o + BLK, :], w2[pl.ds(fo, TF), :], 1, 1)
            hv, gv = _gelu_and_grad(a)
            h[o:o + BLK, pl.ds(fo, TF)] = hv.astype(BF16)
            da[o:o + BLK, pl.ds(fo, TF)] = (gv * dh).astype(BF16)
            return 0

        lax.fori_loop(0, FS // TF, step, 0)

    cw1.wait()
    cw2.wait()
    gx.sb[0].wait_recv()
    gy.sb[0].wait_recv()
    hidden(0)

    for e in (0, -1, 1):
        gx.d2p[e].wait_recv()
        go(gx.d2hp[e])
        gx.d2m[e].wait_recv()
        go(gx.d2hm[e])
    for r in (1, -1):
        gy.d2p[r].wait_recv()
        go(gy.d2hp[r])
        gy.d2m[r].wait_recv()
        go(gy.d2hm[r])
    gx.d2p[2].wait_recv()
    go(gx.d2hp[2])
    gx.d2m[2].wait_recv()
    go(gx.d2hm[2])
    go(gx.sb[1])
    go(gx.sb[-1])
    gy.d2hp[1].wait_recv()
    gy.d2hm[1].wait_recv()
    go(gy.sb[1])
    gy.d2p[2].wait_recv()
    go(gy.d2hp[2])
    gy.d2m[2].wait_recv()
    go(gy.d2hm[2])
    gx.sb[1].wait_recv()
    gy.sb[1].wait_recv()
    hidden(1)
    gy.d2hp[-1].wait_recv()
    gy.d2hm[-1].wait_recv()
    go(gy.sb[-1])
    gx.sb[-1].wait_recv()
    gy.sb[-1].wait_recv()
    hidden(-1)
    for e in REL:
        gx.d2hp[e].wait_recv()
        gx.d2hm[e].wait_recv()
    go(gx.sb[2])
    gy.d2hp[2].wait_recv()
    gy.d2hm[2].wait_recv()
    go(gy.sb[2])
    gx.sb[2].wait_recv()
    gy.sb[2].wait_recv()
    hidden(2)

    live = {}

    def partial_block(k, i):
        s, slot, col, o = k % 2, i % 2, (k % 2) * C, i * BLK

        def step(n, _):
            if k < 2:
                co = pl.multiple_of(col + n * (2 * Q), 2 * Q)
                t = _dot(h[o:o + BLK, :], w2[:, pl.ds(co, 2 * Q)], 1, 0)
            else:
                co = pl.multiple_of(col + n * (2 * Q), 2 * Q)
                t = _dot(da[o:o + BLK, :], w1[pl.ds(co, 2 * Q), :], 1, 1)
            for j in range(2):
                acc[s, 2 * n + j, i] = t[:OWN, j * Q:(j + 1) * Q].reshape(SIDE, R, Q)
                stage[slot, 2 * n + j] = t[OWN:, j * Q:(j + 1) * Q].reshape(SIDE, R, Q)
            return 0

        lax.fori_loop(0, 2, step, 0)

    def partials(k):
        s = k % 2
        if k >= 2:
            for c in live.pop(("p1", k - 2)):
                c.wait_send()
        cs = [remote(stage.at[i % 2], sibr.at[i], sbs.at[i], sbr.at[i], sib) for i in range(SIDE)]

        def add(i):
            cs[i].wait_recv()
            for q in range(4):
                acc[s, q, i] = acc[s, q, i] + sibr[i, q]
            if k < 3:
                pl.semaphore_signal(csib, inc=1, device_id=sib, device_id_type=MESH)

        for i in range(SIDE):
            if i >= 2:
                cs[i - 2].wait_send()
            partial_block(k, i)
            if k > 0:
                pl.semaphore_wait(csib, 1)
            cs[i].start()
            if i >= 1:
                add(i - 1)
        add(SIDE - 1)
        cs[2].wait_send()
        cs[3].wait_send()

    YR, XR = (yp, ym), (xp, xm)

    def ring_copies(get, buf, ss, rs, ring):
        plus, minus = ring
        src = [(get(0, 2), plus), (get(1, 2), minus), (get(1, 1), plus), (get(0, -1), minus), (get(0, 1), plus), (get(1, -1), minus)]
        return [remote(v, buf.at[j], ss.at[j], rs.at[j], d) for j, (v, d) in enumerate(src)]

    def p1_get(k, ab):
        if ab == 0:
            return lambda p, r: acc.at[k % 2, p, IX[r]]
        return lambda p, r: acc.at[k % 2, 2 + p, :, IX[r]]

    def p2_get(k, ab):
        return lambda p, r: zbuf.at[k % 2, 2 * ab + p, IX[r]]

    def e1(k):
        if k >= 2:
            pl.semaphore_wait(c1.at[0], 1)
            pl.semaphore_wait(c1.at[1], 1)
            pl.semaphore_wait(c1.at[2], 1)
            pl.semaphore_wait(c1.at[3], 1)
        s = k % 2
        cs = [ring_copies(p1_get(k, ab), r1.at[s, ab], p1s.at[s, ab], p1r.at[s, ab], (YR, XR)[ab]) for ab in range(2)]
        live["c1", k] = cs
        for j in range(4):
            for ab in range(2):
                cs[ab][j].start()

    def forward(get, buf, cs, ab):
        cs[ab][0].wait_recv()
        v = get(0, 1)
        v[...] = v[...] + buf[ab, 0]
        cs[ab][4].start()
        cs[ab][1].wait_recv()
        v = get(1, -1)
        v[...] = v[...] + buf[ab, 1]
        cs[ab][5].start()

    def final(get, buf, cs, ab):
        for j in (2, 3, 4, 5):
            cs[ab][j].wait_recv()
        return (get(0, 0)[...] + buf[ab, 3] + buf[ab, 4], get(1, 0)[...] + buf[ab, 2] + buf[ab, 5])

    def credit(c):
        for i, d in enumerate((ym, yp, xm, xp)):
            pl.semaphore_signal(c.at[i], inc=1, device_id=d, device_id_type=MESH)

    def e2(k):
        cs = live["c1", k]
        for ab in range(2):
            forward(p1_get(k, ab), r1.at[k % 2], cs, ab)

    def e3(k):
        s = k % 2
        cs = live["c1", k]
        if k >= 2:
            for c in live.pop(("p2", k - 2)):
                c.wait_send()
            for i in range(4):
                pl.semaphore_wait(c2.at[i], 1)
        ds = [ring_copies(p2_get(k, ab), r2.at[s, ab], p2s.at[s, ab], p2r.at[s, ab], (XR, YR)[ab]) for ab in range(2)]
        live["c2", k] = ds
        for ab in range(2):
            a, b = final(p1_get(k, ab), r1.at[s], cs, ab)
            zbuf[s, 2 * ab] = a
            zbuf[s, 2 * ab + 1] = b
            for j in range(4):
                ds[ab][j].start()
        live["p1", k] = [c for v in cs for c in v]
        if k < 2:
            credit(c1)

    def e4(k):
        cs = live["c2", k]
        for ab in range(2):
            forward(p2_get(k, ab), r2.at[k % 2], cs, ab)

    def e5(k):
        cs = live["c2", k]
        for ab in range(2):
            a, b = final(p2_get(k, ab), r2.at[k % 2], cs, ab)
            o = (k % 2) * C + 2 * ab * Q
            ysum[:, o:o + Q] = a
            ysum[:, o + Q:o + 2 * Q] = b
        live["p2", k] = [c for v in cs for c in v]
        if k < 2:
            credit(c2)

    TM = dwst.shape[1]

    def dw2_copy(i):
        r = pl.multiple_of((i // 2) * TM, TM)
        c = pl.multiple_of((i % 2) * FS, FS)
        return pltpu.make_async_copy(dwst.at[i % 2], dw2_hbm.at[pl.ds(r, TM), pl.ds(c, FS)], lsem.at[3 + i % 2])

    def dw1_copy(i):
        r = pl.multiple_of(i * TM, TM)
        return pltpu.make_async_copy(dwst.at[i % 2], dw1_hbm.at[pl.ds(r, TM), :], lsem.at[3 + i % 2])

    def dw2_tile(i):
        r = pl.multiple_of((i // 2) * TM, TM)
        c = pl.multiple_of((i % 2) * FS, FS)
        return _dot(h[:, pl.ds(r, TM)], dy[:, pl.ds(c, FS)], 0, 0)

    def dw1_tile(i):
        r = pl.multiple_of(i * TM, TM)
        return _dot(xn[:, pl.ds(r, TM)], da[...], 0, 0)

    def dw(copy, tile, lo, hi, first):
        def step(i, _):
            @pl.when(i >= first)
            def _():
                copy(i - 2).wait()
            dwst[i % 2] = tile(i)
            copy(i).start()
            return 0

        lax.fori_loop(lo, hi, step, 0)

    NT2 = FS // TM * (D // FS)
    NT1 = D // TM

    partials(0)
    e1(0)
    partials(1)
    e2(0)
    e1(1)
    dw(dw2_copy, dw2_tile, 0, NT2 // 2, 2)
    e3(0)
    partials(2)
    e2(1)
    e1(2)
    e4(0)
    dw(dw2_copy, dw2_tile, NT2 // 2, NT2, 2)
    dw2_copy(NT2 - 2).wait()
    dw2_copy(NT2 - 1).wait()
    e5(0)
    e3(1)
    partials(3)
    e2(2)
    e1(3)
    e4(1)
    dw(dw1_copy, dw1_tile, 0, NT1 // 2, 2)
    e5(1)
    y_out[...] = (x_ref[...].astype(F32) + ysum[...]).astype(BF16)
    e3(2)
    dw(dw1_copy, dw1_tile, NT1 // 2, NT1, 2)
    e2(3)
    e4(2)
    dw1_copy(NT1 - 2).wait()
    dw1_copy(NT1 - 1).wait()
    e5(2)
    e3(3)
    e4(3)
    e5(3)

    xhat, rstd = _ln(x_ref[...].astype(F32))
    dxn = ysum[...]
    gam[0] = jnp.sum(dxn * xhat, axis=0, keepdims=True)
    cs = [remote(gam.at[0], gin.at[0], gs.at[0], gr.at[0], sib)]
    cs += [remote(gam.at[1], gin.at[1 + j], gs.at[1 + j], gr.at[1 + j], d) for j, d in enumerate((xp, xm, xf))]
    cs += [remote(gam.at[2], gin.at[4 + j], gs.at[4 + j], gr.at[4 + j], d) for j, d in enumerate((yp, ym, yf))]
    cs[0].start()
    dxhat = dxn * g_ref[...]
    dx = rstd * (dxhat - jnp.mean(dxhat, axis=-1, keepdims=True) - xhat * jnp.mean(dxhat * xhat, axis=-1, keepdims=True))
    dx_out[...] = (dy[0:R, :].astype(F32) + dx).astype(BF16)
    cs[0].wait_recv()
    gam[1] = gam[0] + gin[0]
    for j in (1, 2, 3):
        cs[j].start()
    for j in (1, 2, 3):
        cs[j].wait_recv()
    gam[2] = gam[1] + gin[1] + gin[2] + gin[3]
    for j in (4, 5, 6):
        cs[j].start()
    for j in (4, 5, 6):
        cs[j].wait_recv()
    dg_out[...] = gam[2] + gin[4] + gin[5] + gin[6]
    for c in cs + pending:
        c.wait_send()
    for key in (("p1", 2), ("p1", 3), ("p2", 2), ("p2", 3)):
        for c in live.pop(key):
            c.wait_send()


def solution(mesh):
    rows = P(("data", "tp"), None)
    assert mesh.shape["tp"] == 2 * SIDE * SIDE

    def body(X, gamma, W1, W2, dY):
        R, D = X.shape
        FS = W1.shape[1]
        T = R * 2 * SIDE * SIDE
        C = D // 2
        Q = C // 4
        vm = pl.BlockSpec(memory_space=pltpu.VMEM)
        anyspace = pl.BlockSpec(memory_space=pl.ANY)
        dma = pltpu.SemaphoreType.DMA
        reg = pltpu.SemaphoreType.REGULAR
        Y, dX, dg, dW1, dW2 = pl.pallas_call(
            _kernel,
            out_shape=(
                jax.ShapeDtypeStruct((R, D), BF16),
                jax.ShapeDtypeStruct((R, D), BF16),
                jax.ShapeDtypeStruct((1, D), F32),
                jax.ShapeDtypeStruct((D, FS), F32),
                jax.ShapeDtypeStruct((FS, D), F32),
            ),
            in_specs=[vm, vm, anyspace, anyspace, anyspace],
            out_specs=(vm, vm, vm, anyspace, anyspace),
            scratch_shapes=[
                pltpu.VMEM((T, D), BF16),
                pltpu.VMEM((T, D), BF16),
                pltpu.VMEM((T, FS), BF16),
                pltpu.VMEM((T, FS), BF16),
                pltpu.VMEM((D, FS), BF16),
                pltpu.VMEM((FS, D), BF16),
                pltpu.VMEM((2, 4, SIDE, SIDE, R, Q), F32),
                pltpu.VMEM((2, 4, SIDE, R, Q), F32),
                pltpu.VMEM((2, 4, SIDE, R, Q), F32),
                pltpu.VMEM((SIDE, 4, SIDE, R, Q), F32),
                pltpu.VMEM((2, 2, 6, SIDE, R, Q), F32),
                pltpu.VMEM((2, 2, 6, R, Q), F32),
                pltpu.VMEM((R, D), F32),
                pltpu.VMEM((3, 1, D), F32),
                pltpu.VMEM((7, 1, D), F32),
                pltpu.VMEM((2, 256, FS), F32),
                dma((48,)), dma((48,)),
                dma((2, 2, 6)), dma((2, 2, 6)),
                dma((2, 2, 6)), dma((2, 2, 6)),
                dma((SIDE,)), dma((SIDE,)),
                dma((7,)), dma((7,)),
                dma((5,)),
                reg((4,)), reg((4,)), reg,
            ],
            compiler_params=pltpu.CompilerParams(
                collective_id=0, has_side_effects=True, vmem_limit_bytes=67043328),
        )(X, gamma.reshape(1, D), W1, W2, dY)
        return Y, dX, dW1, dW2, dg.reshape(D)

    return jax.shard_map(body, mesh=mesh,
                         in_specs=(rows, P(None), P(None, "tp"), P("tp", None), rows),
                         out_specs=(rows, rows, P("data", "tp"), rows, P("data")),
                         check_vma=False)
```

```python
import math

import jax
import jax.numpy as jnp
from jax import lax
from jax.experimental import pallas as pl
from jax.experimental.pallas import tpu as pltpu
from jax.sharding import PartitionSpec as P

EPS = 1e-6
BF16 = jnp.bfloat16
F32 = jnp.float32
MESH = pl.DeviceIdType.MESH

REL = (0, 1, -1, 2)
IX = {0: 0, 1: 1, -1: 2, 2: 3}
ORDER = (0, 1, -1, 2)
SIDE = 4


def _dot(a, b, ca, cb):
    return lax.dot_general(a, b, (((ca,), (cb,)), ((), ())), preferred_element_type=F32)


def _ln(x):
    mu = jnp.mean(x, axis=-1, keepdims=True)
    xc = x - mu
    var = jnp.mean(xc * xc, axis=-1, keepdims=True)
    rstd = lax.rsqrt(var + EPS)
    return xc * rstd, rstd


def _gelu_and_grad(a):
    c = math.sqrt(2.0 / math.pi)
    a2 = a * a
    t = jnp.tanh(c * (a + 0.044715 * (a2 * a)))
    cdf = 0.5 * (1.0 + t)
    grad = cdf + (0.5 * a * (1.0 - t * t)) * (c + (3.0 * 0.044715 * c) * a2)
    return a * cdf, grad


def _kernel(x_ref, g_ref, w1_hbm, w2_hbm, dy_hbm,
            y_out, dx_out, dg_out, dw1_hbm, dw2_hbm,
            xn, dy, h, da, w1, w2, acc, zbuf, stage, sibr, r1, r2, ysum, gam, gin, dwst,
            ags, agr, p1s, p1r, p2s, p2r, sbs, sbr, gs, gr, lsem, c1, c2, csib):
    me = lax.axis_index("tp")
    core = me % 2
    cx = (me // 2) % SIDE
    cy = me // (2 * SIDE)

    def dev(yy, xx, cc):
        return {"tp": ((yy % SIDE) * SIDE + (xx % SIDE)) * 2 + cc}

    yp, ym, yf = dev(cy + 1, cx, core), dev(cy + SIDE - 1, cx, core), dev(cy + 2, cx, core)
    xp, xm, xf = dev(cy, cx + 1, core), dev(cy, cx + SIDE - 1, core), dev(cy, cx + 2, core)
    sib = dev(cy, cx, 1 - core)

    R = x_ref.shape[0]
    HR = R // 2
    D = x_ref.shape[1]
    FS = w1.shape[1]
    BLK = 2 * SIDE * R
    OWN = SIDE * R
    C = D // 2
    Q = C // 4

    cw1 = pltpu.make_async_copy(w1_hbm, w1, lsem.at[0])
    cw2 = pltpu.make_async_copy(w2_hbm, w2, lsem.at[1])
    cdy = pltpu.make_async_copy(dy_hbm, dy.at[pl.ds(0, R)], lsem.at[2])
    cdy.start()
    cw1.start()
    cw2.start()
    xhat, rstd = _ln(x_ref[...].astype(F32))
    xn[0:R, :] = (xhat * g_ref[...]).astype(BF16)

    bar = pltpu.get_barrier_semaphore()
    for d in (yp, ym, yf, xp, xm, xf, sib):
        pl.semaphore_signal(bar, inc=1, device_id=d, device_id_type=MESH)
    pl.semaphore_wait(bar, 7)

    def remote(src, dst, ss, rs, d):
        return pltpu.make_async_remote_copy(src_ref=src, dst_ref=dst, send_sem=ss, recv_sem=rs, device_id=d, device_id_type=MESH)

    pending = []

    def go(*cs):
        for c in cs:
            c.start()
            pending.append(c)

    def got(*cs):
        for c in cs:
            c.wait_recv()

    class Gather:
        def __init__(self, buf, first, second, xfirst, base):
            n = [base]

            def at(a, b, half=None):
                dd, ee = (b, a) if xfirst else (a, b)
                o = (IX[dd] * 2 * SIDE + IX[ee]) * R
                if half is None:
                    return buf.at[pl.ds(o, R)]
                return buf.at[pl.ds(o + half * HR, HR)]

            def mk(src, dst, d):
                i = n[0]
                n[0] += 1
                return remote(src, dst, ags.at[i], agr.at[i], d)

            (fp, fm), (sp, sm) = first, second
            self.d1 = (mk(at(0, 0), at(-1, 0), fp), mk(at(0, 0), at(1, 0), fm))
            self.d1h = (mk(at(-1, 0, 0), at(2, 0, 0), fp), mk(at(1, 0, 1), at(2, 0, 1), fm))
            self.d2 = {r: (mk(at(r, 0), at(r, -1), sp), mk(at(r, 0), at(r, 1), sm)) for r in REL}
            self.d2h = {r: (mk(at(r, -1, 0), at(r, 2, 0), sp), mk(at(r, 1, 1), at(r, 2, 1), sm)) for r in REL}
            self.sb = {r: mk(buf.at[pl.ds(IX[r] * BLK, OWN)], buf.at[pl.ds(IX[r] * BLK + OWN, OWN)], sib) for r in REL}

        def hop1(self):
            for c, n in zip(self.d1, self.d1h):
                got(c)
                go(n)

        def hop2(self, r):
            for c, n in zip(self.d2[r], self.d2h[r]):
                got(c)
                go(n)

    TF = FS // 2

    def keep(dd, f):
        if dd == 1:
            return [[acc.at[1, 2 * f + j, 1 + c] for j in range(2)] for c in range(2)]
        if dd == 2:
            return [[zbuf.at[c, 2 * f + j] for j in range(2)] for c in range(2)]
        return [[dwst.at[c, :, pl.ds(pl.multiple_of(f * TF + j * Q, Q), Q)] for j in range(2)] for c in range(2)]

    def hidden(dd, forward, backward):
        o = IX[dd] * BLK

        def step(f, _):
            fo = pl.multiple_of(f * TF, TF)
            if forward:
                a = _dot(xn[o:o + BLK, :], w1[:, pl.ds(fo, TF)], 1, 0)
                hv, gv = _gelu_and_grad(a)
                h[o:o + BLK, pl.ds(fo, TF)] = hv.astype(BF16)
                if not backward:
                    for c, row in enumerate(keep(dd, f)):
                        for j, ref in enumerate(row):
                            ref[...] = a[c * OWN:(c + 1) * OWN, j * Q:(j + 1) * Q].reshape(ref.shape)
            if backward:
                dh = _dot(dy[o:o + BLK, :], w2[pl.ds(fo, TF), :], 1, 1)
                if forward:
                    da[o:o + BLK, pl.ds(fo, TF)] = (gv * dh).astype(BF16)
                else:
                    for c, row in enumerate(keep(dd, f)):
                        for j, ref in enumerate(row):
                            gv = _gelu_and_grad(ref[...].reshape(OWN, Q))[1]
                            co = pl.multiple_of(fo + j * Q, Q)
                            da[o + c * OWN:o + (c + 1) * OWN, pl.ds(co, Q)] = (
                                gv * dh[c * OWN:(c + 1) * OWN, j * Q:(j + 1) * Q]).astype(BF16)
            return 0

        lax.fori_loop(0, FS // TF, step, 0)

    ROUND = ((0, 0), (1, 0), (1, 1), (0, 1))
    live = {}
    slots = [None, None]
    count = [0]

    def mblk(k, i):
        s, slot, o = k % 2, count[0] % 2, i * BLK
        back, half = ROUND[k]
        count[0] += 1
        if slots[slot] is not None:
            slots[slot].wait_send()

        def step(n, _):
            co = pl.multiple_of(half * C + n * (2 * Q), 2 * Q)
            if back:
                t = _dot(da[o:o + BLK, :], w1[pl.ds(co, 2 * Q), :], 1, 1)
            else:
                t = _dot(h[o:o + BLK, :], w2[:, pl.ds(co, 2 * Q)], 1, 0)
            for j in range(2):
                acc[s, 2 * n + j, i] = t[:OWN, j * Q:(j + 1) * Q].reshape(SIDE, R, Q)
                stage[slot, 2 * n + j] = t[OWN:, j * Q:(j + 1) * Q].reshape(SIDE, R, Q)
            return 0

        lax.fori_loop(0, 2, step, 0)
        if k > 0:
            pl.semaphore_wait(csib.at[i], 1)
        c = remote(stage.at[slot], sibr.at[i], sbs.at[slot], sbr.at[i], sib)
        c.start()
        slots[slot] = c
        live["sib", k, i] = c

    def add(k, i):
        live.pop(("sib", k, i)).wait_recv()
        for q in range(4):
            acc[k % 2, q, i] = acc[k % 2, q, i] + sibr[i, q]
        if k < 3:
            pl.semaphore_signal(csib.at[i], inc=1, device_id=sib, device_id_type=MESH)

    YR, XR = (yp, ym), (xp, xm)

    def ring_copies(get, buf, ss, rs, ring, parts=1):
        plus, minus = ring
        src = [(get(0, 2), plus), (get(1, 2), minus), (get(1, 1), plus), (get(0, -1), minus), (get(0, 1), plus), (get(1, -1), minus)]
        out = []
        for j, (v, d) in enumerate(src):
            if parts == 1 or j > 3:
                out.append([remote(v, buf.at[j], ss.at[j, 0], rs.at[j, 0], d)])
            else:
                n = SIDE // parts
                out.append([remote(v.at[pl.ds(c * n, n)], buf.at[j, pl.ds(c * n, n)], ss.at[j, c], rs.at[j, c], d) for c in range(parts)])
        return out

    def p1_get(k, ab):
        if ab == 0:
            return lambda p, r: acc.at[k % 2, p, IX[r]]
        return lambda p, r: acc.at[k % 2, 2 + p, :, IX[r]]

    def p2_get(k, ab):
        return lambda p, r: zbuf.at[k % 2, 2 * ab + p, IX[r]]

    def begin(k):
        if k >= 2:
            for i in range(4):
                pl.semaphore_wait(c1.at[i], 1)
        s = k % 2
        live["c1", k] = [ring_copies(p1_get(k, ab), r1.at[s, ab], p1s.at[s, ab], p1r.at[s, ab], (YR, XR)[ab], 1 + ab) for ab in range(2)]

    def send_a(k, js):
        for j in js:
            live["c1", k][0][j][0].start()

    def send_b(k, c):
        for j in range(4):
            live["c1", k][1][j][c].start()

    def e1(k):
        begin(k)
        for j in range(4):
            send_a(k, (j,))
            for c in live["c1", k][1][j]:
                c.start()

    def forward(get, buf, cs, ab):
        for j, p, r in ((0, 0, 1), (1, 1, -1)):
            got(*cs[ab][j])
            v = get(p, r)
            v[...] = v[...] + buf[ab, j]
            cs[ab][4 + j][0].start()

    def final(get, buf, cs, ab):
        for j in (2, 3, 4, 5):
            got(*cs[ab][j])
        return (get(0, 0)[...] + buf[ab, 3] + buf[ab, 4], get(1, 0)[...] + buf[ab, 2] + buf[ab, 5])

    def credit(c):
        for i, d in enumerate((ym, yp, xm, xp)):
            pl.semaphore_signal(c.at[i], inc=1, device_id=d, device_id_type=MESH)

    def drained(key):
        for v in live.pop(key):
            for cs in v:
                for c in cs:
                    c.wait_send()

    def e2(k):
        for ab in range(2):
            forward(p1_get(k, ab), r1.at[k % 2], live["c1", k], ab)

    def e3(k):
        s = k % 2
        if k >= 2:
            drained(("c2", k - 2))
            for i in range(4):
                pl.semaphore_wait(c2.at[i], 1)
        ds = [ring_copies(p2_get(k, ab), r2.at[s, ab], p2s.at[s, ab], p2r.at[s, ab], (XR, YR)[ab]) for ab in range(2)]
        live["c2", k] = ds
        for ab in range(2):
            a, b = final(p1_get(k, ab), r1.at[s], live["c1", k], ab)
            zbuf[s, 2 * ab] = a
            zbuf[s, 2 * ab + 1] = b
            for j in range(4):
                ds[ab][j][0].start()
        if k < 2:
            credit(c1)

    def e4(k):
        for ab in range(2):
            forward(p2_get(k, ab), r2.at[k % 2], live["c2", k], ab)

    def e5(k):
        back, half = ROUND[k]
        for ab in range(2):
            a, b = final(p2_get(k, ab), r2.at[k % 2], live["c2", k], ab)
            o = half * C + 2 * ab * Q
            ysum[back, :, o:o + Q] = a
            ysum[back, :, o + Q:o + 2 * Q] = b
        if k < 2:
            credit(c2)

    TM = dwst.shape[1]
    NT2 = FS // TM * (D // FS)
    NT1 = D // TM

    def dw2_copy(i):
        r = pl.multiple_of((i // 2) * TM, TM)
        c = pl.multiple_of((i % 2) * FS, FS)
        return pltpu.make_async_copy(dwst.at[i % 2], dw2_hbm.at[pl.ds(r, TM), pl.ds(c, FS)], lsem.at[3 + i % 2])

    def dw1_copy(i):
        r = pl.multiple_of(i * TM, TM)
        return pltpu.make_async_copy(dwst.at[i % 2], dw1_hbm.at[pl.ds(r, TM), :], lsem.at[3 + i % 2])

    def dw2_tile(i):
        r = pl.multiple_of((i // 2) * TM, TM)
        c = pl.multiple_of((i % 2) * FS, FS)
        return _dot(h[:, pl.ds(r, TM)], dy[:, pl.ds(c, FS)], 0, 0)

    def dw1_tile(i):
        r = pl.multiple_of(i * TM, TM)
        return _dot(xn[:, pl.ds(r, TM)], da[...], 0, 0)

    done = [0]

    def dw(n):
        i0 = done[0]
        done[0] += n
        copy, tile, lo, total = (dw2_copy, dw2_tile, i0, NT2) if i0 < NT2 else (dw1_copy, dw1_tile, i0 - NT2, NT1)
        hi = lo + n
        assert hi <= total

        def step(i, _):
            @pl.when(i >= 2)
            def _():
                copy(i - 2).wait()
            dwst[i % 2] = tile(i)
            copy(i).start()
            return 0

        lax.fori_loop(lo, hi, step, 0)
        if hi == total:
            copy(total - 2).wait()
            copy(total - 1).wait()

    gx = Gather(xn, (xp, xm), (yp, ym), True, 0)
    gy = Gather(dy, (yp, ym), (xp, xm), False, 24)

    cdy.wait()
    go(*gx.d1, *gy.d1)
    go(*gx.d2[0], *gy.d2[0])
    gx.hop1()
    gy.hop1()
    go(*gx.d2[-1], *gx.d2[1])
    gy.hop2(0)
    go(*gy.d2[1], *gy.d2[-1])
    got(*gx.d1h)
    go(*gx.d2[2], gx.sb[0])
    got(*gy.d2h[0])
    go(gy.sb[0])
    got(*gy.d1h)
    cw1.wait()
    cw2.wait()
    got(gx.sb[0], gy.sb[0])
    hidden(0, True, True)
    gy.hop2(1)
    go(*gy.d2[2])
    gx.hop2(0)
    gx.hop2(-1)
    mblk(0, 0)
    gx.hop2(1)
    add(0, 0)
    mblk(1, 0)
    gy.hop2(-1)
    add(1, 0)
    gx.hop2(2)
    go(gx.sb[1], gx.sb[-1])
    got(*gy.d2h[1])
    go(gy.sb[1])
    got(gx.sb[1])
    hidden(1, True, False)
    gy.hop2(2)
    mblk(0, 1)
    got(gx.sb[-1])
    hidden(-1, True, False)
    add(0, 1)
    begin(0)
    send_b(0, 0)
    mblk(0, 2)
    got(*gy.d2h[-1])
    go(gy.sb[-1])
    got(gy.sb[1])
    hidden(1, False, True)
    add(0, 2)
    send_a(0, (2, 3))
    for r in REL:
        got(*gx.d2h[r])
    go(gx.sb[2])
    got(*gy.d2h[2])
    go(gy.sb[2])
    got(gx.sb[2])
    hidden(2, True, False)
    mblk(0, 3)
    got(gy.sb[-1])
    hidden(-1, False, True)
    add(0, 3)
    send_a(0, (0, 1))
    send_b(0, 1)
    got(gy.sb[2])
    hidden(2, False, True)
    mblk(1, 1)
    e2(0)
    mblk(1, 2)
    add(1, 1)
    mblk(1, 3)
    add(1, 2)
    dw(2)
    add(1, 3)
    e1(1)
    e3(0)
    drained(("c1", 0))
    mblk(2, 0)
    mblk(2, 1)
    add(2, 0)
    mblk(2, 2)
    add(2, 1)
    e2(1)
    mblk(2, 3)
    add(2, 2)
    dw(2)
    add(2, 3)
    e1(2)
    e4(0)
    dw(2)
    e3(1)
    drained(("c1", 1))
    mblk(3, 0)
    mblk(3, 1)
    add(3, 0)
    mblk(3, 2)
    add(3, 1)
    mblk(3, 3)
    add(3, 2)
    dw(2)
    add(3, 3)
    e1(3)
    e2(2)
    e5(0)
    e4(1)
    dw(2)
    e3(2)
    e2(3)
    dw(2)
    e5(1)
    e4(2)
    e3(3)
    dw(2)

    xhat, rstd = _ln(x_ref[...].astype(F32))
    e5(2)
    dxn = ysum[1]
    gam[0] = jnp.sum(dxn * xhat, axis=0, keepdims=True)
    cs = [remote(gam.at[0], gin.at[0], gs.at[0], gr.at[0], sib)]
    cs += [remote(gam.at[1], gin.at[1 + j], gs.at[1 + j], gr.at[1 + j], d) for j, d in enumerate((xp, xm, xf))]
    cs += [remote(gam.at[2], gin.at[4 + j], gs.at[4 + j], gr.at[4 + j], d) for j, d in enumerate((yp, ym, yf))]
    go(cs[0])
    dxhat = dxn * g_ref[...]
    dx = rstd * (dxhat - jnp.mean(dxhat, axis=-1, keepdims=True) - xhat * jnp.mean(dxhat * xhat, axis=-1, keepdims=True))
    dx_out[...] = (dy[0:R, :].astype(F32) + dx).astype(BF16)
    got(cs[0])
    gam[1] = gam[0] + gin[0]
    go(*cs[1:4])
    e4(3)
    got(*cs[1:4])
    gam[2] = gam[1] + gin[1] + gin[2] + gin[3]
    go(*cs[4:7])
    dw(2)
    got(*cs[4:7])
    dg_out[...] = gam[2] + gin[4] + gin[5] + gin[6]
    e5(3)
    y_out[...] = (x_ref[...].astype(F32) + ysum[0]).astype(BF16)
    for c in pending + [v for v in slots]:
        c.wait_send()
    for key in (("c1", 2), ("c1", 3), ("c2", 2), ("c2", 3)):
        drained(key)


def _out_kernel(*refs):
    n = (len(refs) - 1) // 3
    src, dst, buf, sem = refs[:n], refs[n:2 * n], refs[2 * n:3 * n], refs[3 * n]
    reads, writes = [], []
    for s, d, b in zip(src, dst, buf):
        m = max(1, s.shape[0] * s.shape[1] * s.dtype.itemsize // 2 ** 20)
        r = s.shape[0] // m
        for i in range(m):
            j = len(reads)
            part = pl.ds(i * r, r)
            reads.append(pltpu.make_async_copy(s.at[part], b.at[part], sem.at[0, j]))
            writes.append(pltpu.make_async_copy(b.at[part], d.at[part], sem.at[1, j]))
    for c in reads:
        c.start()
    for c, w in zip(reads, writes):
        c.wait()
        w.start()
    for w in writes:
        w.wait()


def solution(mesh):
    rows = P(("data", "tp"), None)
    assert mesh.shape["tp"] == 2 * SIDE * SIDE

    def body(X, gamma, W1, W2, dY):
        R, D = X.shape
        FS = W1.shape[1]
        T = R * 2 * SIDE * SIDE
        C = D // 2
        Q = C // 4
        vm = pl.BlockSpec(memory_space=pltpu.VMEM)
        anyspace = pl.BlockSpec(memory_space=pl.ANY)
        dma = pltpu.SemaphoreType.DMA
        reg = pltpu.SemaphoreType.REGULAR
        raw = pl.pallas_call(
            _kernel,
            out_shape=(
                jax.ShapeDtypeStruct((R, D), BF16),
                jax.ShapeDtypeStruct((R, D), BF16),
                jax.ShapeDtypeStruct((1, D), F32),
                jax.ShapeDtypeStruct((D, FS), F32),
                jax.ShapeDtypeStruct((FS, D), F32),
            ),
            in_specs=[vm, vm, anyspace, anyspace, anyspace],
            out_specs=(vm, vm, vm, anyspace, anyspace),
            scratch_shapes=[
                pltpu.VMEM((T, D), BF16),
                pltpu.VMEM((T, D), BF16),
                pltpu.VMEM((T, FS), BF16),
                pltpu.VMEM((T, FS), BF16),
                pltpu.VMEM((D, FS), BF16),
                pltpu.VMEM((FS, D), BF16),
                pltpu.VMEM((2, 4, SIDE, SIDE, R, Q), F32),
                pltpu.VMEM((2, 4, SIDE, R, Q), F32),
                pltpu.VMEM((2, 4, SIDE, R, Q), F32),
                pltpu.VMEM((SIDE, 4, SIDE, R, Q), F32),
                pltpu.VMEM((2, 2, 6, SIDE, R, Q), F32),
                pltpu.VMEM((2, 2, 6, R, Q), F32),
                pltpu.VMEM((2, R, D), F32),
                pltpu.VMEM((3, 1, D), F32),
                pltpu.VMEM((7, 1, D), F32),
                pltpu.VMEM((2, 256, FS), F32),
                dma((48,)), dma((48,)),
                dma((2, 2, 6, 2)), dma((2, 2, 6, 2)),
                dma((2, 2, 6, 1)), dma((2, 2, 6, 1)),
                dma((2,)), dma((SIDE,)),
                dma((7,)), dma((7,)),
                dma((5,)),
                reg((4,)), reg((4,)), reg((SIDE,)),
            ],
            compiler_params=pltpu.CompilerParams(
                collective_id=0, has_side_effects=True, vmem_limit_bytes=67043328),
        )(X, gamma.reshape(1, D), W1, W2, dY)
        Y, dX, dg, dW1, dW2 = pl.pallas_call(
            _out_kernel,
            out_shape=tuple(jax.ShapeDtypeStruct(v.shape, v.dtype) for v in raw),
            in_specs=[anyspace] * 5,
            out_specs=(anyspace,) * 5,
            scratch_shapes=[pltpu.VMEM(v.shape, v.dtype) for v in raw] + [dma((2, 32))],
        )(*raw)
        return Y, dX, dW1, dW2, dg.reshape(D)

    return jax.shard_map(body, mesh=mesh,
                         in_specs=(rows, P(None), P(None, "tp"), P("tp", None), rows),
                         out_specs=(rows, rows, P("data", "tp"), rows, P("data")),
                         check_vma=False)
```

```python
import math

import jax
import jax.numpy as jnp
from jax import lax
from jax.experimental import pallas as pl
from jax.experimental.pallas import tpu as pltpu
from jax.sharding import PartitionSpec as P

EPS = 1e-6
BF16 = jnp.bfloat16
F32 = jnp.float32
MESH = pl.DeviceIdType.MESH

REL = (0, 1, -1, 2)
IX = {0: 0, 1: 1, -1: 2, 2: 3}
ORDER = (0, 1, -1, 2)
SIDE = 4


def _dot(a, b, ca, cb):
    return lax.dot_general(a, b, (((ca,), (cb,)), ((), ())), preferred_element_type=F32)


def _ln(x):
    mu = jnp.mean(x, axis=-1, keepdims=True)
    xc = x - mu
    var = jnp.mean(xc * xc, axis=-1, keepdims=True)
    rstd = lax.rsqrt(var + EPS)
    return xc * rstd, rstd


def _gelu_and_grad(a):
    c = math.sqrt(2.0 / math.pi)
    a2 = a * a
    t = jnp.tanh(c * (a + 0.044715 * (a2 * a)))
    cdf = 0.5 * (1.0 + t)
    grad = cdf + (0.5 * a * (1.0 - t * t)) * (c + (3.0 * 0.044715 * c) * a2)
    return a * cdf, grad


def _kernel(x_ref, g_ref, w1_hbm, w2_hbm, dy_hbm,
            y_out, dx_out, dg_out, dw1_hbm, dw2_hbm,
            xn, dy, h, da, w1, w2, acc, zbuf, stage, sibr, r1, r2, ysum, gam, gin, dwst,
            ags, agr, p1s, p1r, p2s, p2r, sbs, sbr, gs, gr, lsem, c1, c2, csib):
    me = lax.axis_index("tp")
    core = me % 2
    cx = (me // 2) % SIDE
    cy = me // (2 * SIDE)

    def dev(yy, xx, cc):
        return {"tp": ((yy % SIDE) * SIDE + (xx % SIDE)) * 2 + cc}

    yp, ym, yf = dev(cy + 1, cx, core), dev(cy + SIDE - 1, cx, core), dev(cy + 2, cx, core)
    xp, xm, xf = dev(cy, cx + 1, core), dev(cy, cx + SIDE - 1, core), dev(cy, cx + 2, core)
    sib = dev(cy, cx, 1 - core)

    R = x_ref.shape[0]
    HR = R // 2
    D = x_ref.shape[1]
    FS = w1.shape[1]
    BLK = 2 * SIDE * R
    OWN = SIDE * R
    C = D // 2
    Q = C // 4

    cw1 = pltpu.make_async_copy(w1_hbm, w1, lsem.at[0])
    cw2 = pltpu.make_async_copy(w2_hbm, w2, lsem.at[1])
    cdy = pltpu.make_async_copy(dy_hbm, dy.at[pl.ds(0, R)], lsem.at[2])
    cdy.start()
    cw1.start()
    cw2.start()
    xhat, rstd = _ln(x_ref[...].astype(F32))
    xn[0:R, :] = (xhat * g_ref[...]).astype(BF16)

    bar = pltpu.get_barrier_semaphore()
    for d in (yp, ym, yf, xp, xm, xf, sib):
        pl.semaphore_signal(bar, inc=1, device_id=d, device_id_type=MESH)
    pl.semaphore_wait(bar, 7)

    def remote(src, dst, ss, rs, d):
        return pltpu.make_async_remote_copy(src_ref=src, dst_ref=dst, send_sem=ss, recv_sem=rs, device_id=d, device_id_type=MESH)

    pending = []

    def go(*cs):
        for c in cs:
            c.start()
            pending.append(c)

    def got(*cs):
        for c in cs:
            c.wait_recv()

    class Half:
        def __init__(self, buf, col, first, second, xfirst, base):
            n = [base]

            def at(a, b, half=None):
                dd, ee = (b, a) if xfirst else (a, b)
                o = (IX[dd] * 2 * SIDE + IX[ee]) * R
                if half is None:
                    return buf.at[pl.ds(o, R), pl.ds(col, C)]
                return buf.at[pl.ds(o + half * HR, HR), pl.ds(col, C)]

            def mk(src, dst, d):
                i = n[0]
                n[0] += 1
                return remote(src, dst, ags.at[i], agr.at[i], d)

            (fp, fm), (sp, sm) = first, second
            self.d1 = (mk(at(0, 0), at(-1, 0), fp), mk(at(0, 0), at(1, 0), fm))
            self.d1h = (mk(at(-1, 0, 0), at(2, 0, 0), fp), mk(at(1, 0, 1), at(2, 0, 1), fm))
            self.d2 = {r: (mk(at(r, 0), at(r, -1), sp), mk(at(r, 0), at(r, 1), sm)) for r in REL}
            self.d2h = {r: (mk(at(r, -1, 0), at(r, 2, 0), sp), mk(at(r, 1, 1), at(r, 2, 1), sm)) for r in REL}

        def hop1(self):
            for c, n in zip(self.d1, self.d1h):
                got(c)
                go(n)

        def hop2(self, r):
            for c, n in zip(self.d2[r], self.d2h[r]):
                got(c)
                go(n)

    class Gather:
        def __init__(self, buf, base):
            self.xy = Half(buf, 0, (xp, xm), (yp, ym), True, base)
            self.yx = Half(buf, C, (yp, ym), (xp, xm), False, base + 20)
            self.sb = {r: tuple(remote(buf.at[pl.ds(IX[r] * BLK + o, n)], buf.at[pl.ds(IX[r] * BLK + OWN + o, n)],
                                       ags.at[base + 40 + 2 * IX[r] + j], agr.at[base + 40 + 2 * IX[r] + j], sib)
                                for j, (o, n) in enumerate(((0, OWN - R), (OWN - R, R)))) for r in REL}

        def s0(self):
            go(*self.xy.d1, *self.yx.d1, *self.xy.d2[0], *self.yx.d2[0])

        def s1(self):
            self.xy.hop1()
            self.yx.hop1()

        def s1b(self):
            for r in (1, -1):
                go(*self.xy.d2[r], *self.yx.d2[r])

        def s2(self):
            self.xy.hop2(0)
            self.yx.hop2(0)
            go(self.sb[0][0])

        def s3(self):
            got(*self.xy.d1h, *self.yx.d1h)
            go(*self.xy.d2[2], *self.yx.d2[2])

        def s4(self):
            got(*self.yx.d2h[0])
            go(self.sb[0][1])

        def s5(self):
            for r in (1, -1):
                self.xy.hop2(r)
                self.yx.hop2(r)
            go(self.sb[1][0], self.sb[-1][0])

        def s6(self):
            self.xy.hop2(2)
            self.yx.hop2(2)

        def s7(self):
            for r in (1, -1):
                got(*self.yx.d2h[r])
                go(self.sb[r][1])

        def s8(self):
            got(*self.xy.d2h[0], *self.xy.d2h[1], *self.xy.d2h[-1])
            go(self.sb[2][0])
            got(*self.xy.d2h[2], *self.yx.d2h[2])
            go(self.sb[2][1])

    TF = FS // 2

    def keep(dd, f):
        if dd in (0, 1):
            return [[acc.at[1, 2 * f + j, (0, 3)[c] if dd == 0 else (1, 2)[c]] for j in range(2)] for c in range(2)]
        if dd == 2:
            return [[zbuf.at[c, 2 * f + j] for j in range(2)] for c in range(2)]
        return [[dwst.at[c, :, pl.ds(pl.multiple_of(f * TF + j * Q, Q), Q)] for j in range(2)] for c in range(2)]

    def forward_h(dd):
        o = IX[dd] * BLK

        def step(f, _):
            fo = pl.multiple_of(f * TF, TF)
            a = _dot(xn[o:o + BLK, :], w1[:, pl.ds(fo, TF)], 1, 0)
            hv, gv = _gelu_and_grad(a)
            h[o:o + BLK, pl.ds(fo, TF)] = hv.astype(BF16)
            for c, row in enumerate(keep(dd, f)):
                for j, ref in enumerate(row):
                    ref[...] = gv[c * OWN:(c + 1) * OWN, j * Q:(j + 1) * Q].reshape(ref.shape)
            return 0

        lax.fori_loop(0, FS // TF, step, 0)

    def backward_h(dd):
        o = IX[dd] * BLK

        def step(f, _):
            fo = pl.multiple_of(f * TF, TF)
            dh = _dot(dy[o:o + BLK, :], w2[pl.ds(fo, TF), :], 1, 1)
            for c, row in enumerate(keep(dd, f)):
                for j, ref in enumerate(row):
                    co = pl.multiple_of(fo + j * Q, Q)
                    da[o + c * OWN:o + (c + 1) * OWN, pl.ds(co, Q)] = (
                        ref[...].reshape(OWN, Q) * dh[c * OWN:(c + 1) * OWN, j * Q:(j + 1) * Q]).astype(BF16)
            return 0

        lax.fori_loop(0, FS // TF, step, 0)

    ROUND = ((0, 0), (1, 0), (1, 1), (0, 1))
    live = {}
    slots = [None, None]
    count = [0]

    def mblk(k, i):
        s, slot, o = k % 2, count[0] % 2, i * BLK
        back, half = ROUND[k]
        count[0] += 1
        if slots[slot] is not None:
            slots[slot].wait_send()

        def step(n, _):
            co = pl.multiple_of(half * C + n * (2 * Q), 2 * Q)
            if back:
                t = _dot(da[o:o + BLK, :], w1[pl.ds(co, 2 * Q), :], 1, 1)
            else:
                t = _dot(h[o:o + BLK, :], w2[:, pl.ds(co, 2 * Q)], 1, 0)
            for j in range(2):
                acc[s, 2 * n + j, i] = t[:OWN, j * Q:(j + 1) * Q].reshape(SIDE, R, Q)
                stage[slot, 2 * n + j] = t[OWN:, j * Q:(j + 1) * Q].reshape(SIDE, R, Q)
            return 0

        lax.fori_loop(0, 2, step, 0)
        if k > 0:
            pl.semaphore_wait(csib.at[i], 1)
        c = remote(stage.at[slot], sibr.at[i], sbs.at[slot], sbr.at[i], sib)
        c.start()
        slots[slot] = c
        live["sib", k, i] = c

    def add(k, i):
        live.pop(("sib", k, i)).wait_recv()
        for q in range(4):
            acc[k % 2, q, i] = acc[k % 2, q, i] + sibr[i, q]
        if k < 3:
            pl.semaphore_signal(csib.at[i], inc=1, device_id=sib, device_id_type=MESH)

    YR, XR = (yp, ym), (xp, xm)

    def ring_copies(get, buf, ss, rs, ring):
        plus, minus = ring
        src = [(get(0, 2), plus), (get(1, 2), minus), (get(1, 1), plus), (get(0, -1), minus), (get(0, 1), plus), (get(1, -1), minus)]
        return [[remote(v, buf.at[j], ss.at[j], rs.at[j], d)] for j, (v, d) in enumerate(src)]

    def p1_get(k, ab):
        if ab == 0:
            return lambda p, r: acc.at[k % 2, p, IX[r]]
        return lambda p, r: acc.at[k % 2, 2 + p, :, IX[r]]

    def p2_get(k, ab):
        return lambda p, r: zbuf.at[k % 2, 2 * ab + p, IX[r]]

    def begin(k):
        if k >= 2:
            for i in range(4):
                pl.semaphore_wait(c1.at[i], 1)
        s = k % 2
        live["c1", k] = [ring_copies(p1_get(k, ab), r1.at[s, ab], p1s.at[s, ab], p1r.at[s, ab], (YR, XR)[ab]) for ab in range(2)]

    def send_p1(k, js):
        for j in js:
            for ab in range(2):
                for c in live["c1", k][ab][j]:
                    c.start()

    def e1(k):
        begin(k)
        send_p1(k, range(4))

    def forward(get, buf, cs, ab):
        for j, p, r in ((0, 0, 1), (1, 1, -1)):
            got(*cs[ab][j])
            v = get(p, r)
            v[...] = v[...] + buf[ab, j]
            cs[ab][4 + j][0].start()

    def final(get, buf, cs, ab):
        for j in (2, 3, 4, 5):
            got(*cs[ab][j])
        return (get(0, 0)[...] + buf[ab, 3] + buf[ab, 4], get(1, 0)[...] + buf[ab, 2] + buf[ab, 5])

    def credit(c):
        for i, d in enumerate((ym, yp, xm, xp)):
            pl.semaphore_signal(c.at[i], inc=1, device_id=d, device_id_type=MESH)

    def drained(key):
        for v in live.pop(key):
            for cs in v:
                for c in cs:
                    c.wait_send()

    def e2(k, abs_=(0, 1)):
        for ab in abs_:
            forward(p1_get(k, ab), r1.at[k % 2], live["c1", k], ab)

    def e3(k):
        s = k % 2
        if k >= 2:
            drained(("c2", k - 2))
            for i in range(4):
                pl.semaphore_wait(c2.at[i], 1)
        ds = [ring_copies(p2_get(k, ab), r2.at[s, ab], p2s.at[s, ab], p2r.at[s, ab], (XR, YR)[ab]) for ab in range(2)]
        live["c2", k] = ds
        for ab in range(2):
            a, b = final(p1_get(k, ab), r1.at[s], live["c1", k], ab)
            zbuf[s, 2 * ab] = a
            zbuf[s, 2 * ab + 1] = b
            for j in range(4):
                ds[ab][j][0].start()
        if k < 2:
            credit(c1)

    def e4(k):
        for ab in range(2):
            forward(p2_get(k, ab), r2.at[k % 2], live["c2", k], ab)

    def e5(k):
        back, half = ROUND[k]
        for ab in range(2):
            a, b = final(p2_get(k, ab), r2.at[k % 2], live["c2", k], ab)
            o = half * C + 2 * ab * Q
            ysum[back, :, o:o + Q] = a
            ysum[back, :, o + Q:o + 2 * Q] = b
        if k < 2:
            credit(c2)

    TM = dwst.shape[1]
    NT2 = FS // TM * (D // FS)
    NT1 = D // TM

    def dw2_copy(i):
        r = pl.multiple_of((i // 2) * TM, TM)
        c = pl.multiple_of((i % 2) * FS, FS)
        return pltpu.make_async_copy(dwst.at[i % 2], dw2_hbm.at[pl.ds(r, TM), pl.ds(c, FS)], lsem.at[3 + i % 2])

    def dw1_copy(i):
        r = pl.multiple_of(i * TM, TM)
        return pltpu.make_async_copy(dwst.at[i % 2], dw1_hbm.at[pl.ds(r, TM), :], lsem.at[3 + i % 2])

    def dw2_tile(i):
        r = pl.multiple_of((i // 2) * TM, TM)
        c = pl.multiple_of((i % 2) * FS, FS)
        return _dot(h[:, pl.ds(r, TM)], dy[:, pl.ds(c, FS)], 0, 0)

    def dw1_tile(i):
        r = pl.multiple_of(i * TM, TM)
        return _dot(xn[:, pl.ds(r, TM)], da[...], 0, 0)

    done = [0]

    def dw(n):
        i0 = done[0]
        done[0] += n
        copy, tile, lo, total = (dw2_copy, dw2_tile, i0, NT2) if i0 < NT2 else (dw1_copy, dw1_tile, i0 - NT2, NT1)
        hi = lo + n
        assert hi <= total

        def step(i, _):
            @pl.when(i >= 2)
            def _():
                copy(i - 2).wait()
            dwst[i % 2] = tile(i)
            copy(i).start()
            return 0

        lax.fori_loop(lo, hi, step, 0)
        if hi == total:
            copy(total - 2).wait()
            copy(total - 1).wait()

    gx = Gather(xn, 0)
    gy = Gather(dy, 48)

    gx.s0()
    gx.s1()
    gx.s2()
    gx.s1b()
    gx.s3()
    gx.s4()
    cw1.wait()
    got(*gx.sb[0])
    forward_h(0)
    gx.s5()
    cw2.wait()
    mblk(0, 0)
    gx.s6()
    cdy.wait()
    gy.s0()
    gx.s7()
    gx.s8()
    add(0, 0)
    got(*gx.sb[1])
    forward_h(1)
    gy.s1()
    gy.s2()
    gy.s1b()
    mblk(0, 1)
    got(*gx.sb[-1])
    forward_h(-1)
    gy.s3()
    mblk(0, 2)
    add(0, 1)
    got(*gx.sb[2])
    forward_h(2)
    add(0, 2)
    gy.s4()
    mblk(0, 3)
    gy.s5()
    got(*gy.sb[0])
    backward_h(0)
    add(0, 3)
    gy.s6()
    e1(0)
    mblk(1, 0)
    gy.s7()
    gy.s8()
    got(*gy.sb[1])
    backward_h(1)
    add(1, 0)
    mblk(1, 1)
    got(*gy.sb[-1])
    backward_h(-1)
    add(1, 1)
    e2(0)
    mblk(1, 2)
    got(*gy.sb[2])
    backward_h(2)
    add(1, 2)
    mblk(1, 3)
    dw(2)
    add(1, 3)
    e1(1)
    e3(0)
    drained(("c1", 0))
    mblk(2, 0)
    mblk(2, 1)
    add(2, 0)
    mblk(2, 2)
    add(2, 1)
    e2(1)
    mblk(2, 3)
    add(2, 2)
    dw(2)
    add(2, 3)
    e1(2)
    e4(0)
    dw(2)
    e3(1)
    drained(("c1", 1))
    mblk(3, 0)
    mblk(3, 1)
    add(3, 0)
    mblk(3, 2)
    add(3, 1)
    mblk(3, 3)
    add(3, 2)
    dw(2)
    add(3, 3)
    e2(2)
    e4(1)
    begin(3)
    send_p1(3, (0, 1))
    e5(0)
    dw(4)
    e3(2)
    send_p1(3, (2, 3))
    dw(2)
    e5(1)
    e4(2)
    e2(3)
    dw(2)

    xhat, rstd = _ln(x_ref[...].astype(F32))
    e5(2)
    dxn = ysum[1]
    gam[0] = jnp.sum(dxn * xhat, axis=0, keepdims=True)
    cs = [remote(gam.at[0], gin.at[0], gs.at[0], gr.at[0], sib)]
    cs += [remote(gam.at[1], gin.at[1 + j], gs.at[1 + j], gr.at[1 + j], d) for j, d in enumerate((xp, xm, xf))]
    cs += [remote(gam.at[2], gin.at[4 + j], gs.at[4 + j], gr.at[4 + j], d) for j, d in enumerate((yp, ym, yf))]
    go(cs[0])
    e3(3)
    dxhat = dxn * g_ref[...]
    dx = rstd * (dxhat - jnp.mean(dxhat, axis=-1, keepdims=True) - xhat * jnp.mean(dxhat * xhat, axis=-1, keepdims=True))
    dx_out[...] = (dy[0:R, :].astype(F32) + dx).astype(BF16)
    got(cs[0])
    gam[1] = gam[0] + gin[0]
    go(*cs[1:4])
    e4(3)
    got(*cs[1:4])
    gam[2] = gam[1] + gin[1] + gin[2] + gin[3]
    go(*cs[4:7])
    e5(3)
    y_out[...] = (x_ref[...].astype(F32) + ysum[0]).astype(BF16)
    got(*cs[4:7])
    dg_out[...] = gam[2] + gin[4] + gin[5] + gin[6]
    for c in pending + [v for v in slots]:
        c.wait_send()
    for key in (("c1", 2), ("c1", 3), ("c2", 2), ("c2", 3)):
        drained(key)


def _out_kernel(*refs):
    n = (len(refs) - 1) // 3
    src, dst, buf, sem = refs[:n], refs[n:2 * n], refs[2 * n:3 * n], refs[3 * n]
    reads, writes = [], []
    for s, d, b in zip(src, dst, buf):
        m = max(1, s.shape[0] * s.shape[1] * s.dtype.itemsize // 2 ** 20)
        r = s.shape[0] // m
        for i in range(m):
            j = len(reads)
            part = pl.ds(i * r, r)
            reads.append(pltpu.make_async_copy(s.at[part], b.at[part], sem.at[0, j]))
            writes.append(pltpu.make_async_copy(b.at[part], d.at[part], sem.at[1, j]))
    for c in reads:
        c.start()
    for c, w in zip(reads, writes):
        c.wait()
        w.start()
    for w in writes:
        w.wait()


def solution(mesh):
    rows = P(("data", "tp"), None)
    assert mesh.shape["tp"] == 2 * SIDE * SIDE

    def body(X, gamma, W1, W2, dY):
        R, D = X.shape
        FS = W1.shape[1]
        T = R * 2 * SIDE * SIDE
        C = D // 2
        Q = C // 4
        vm = pl.BlockSpec(memory_space=pltpu.VMEM)
        anyspace = pl.BlockSpec(memory_space=pl.ANY)
        dma = pltpu.SemaphoreType.DMA
        reg = pltpu.SemaphoreType.REGULAR
        raw = pl.pallas_call(
            _kernel,
            out_shape=(
                jax.ShapeDtypeStruct((R, D), BF16),
                jax.ShapeDtypeStruct((R, D), BF16),
                jax.ShapeDtypeStruct((1, D), F32),
                jax.ShapeDtypeStruct((D, FS), F32),
                jax.ShapeDtypeStruct((FS, D), F32),
            ),
            in_specs=[vm, vm, anyspace, anyspace, anyspace],
            out_specs=(vm, vm, vm, anyspace, anyspace),
            scratch_shapes=[
                pltpu.VMEM((T, D), BF16),
                pltpu.VMEM((T, D), BF16),
                pltpu.VMEM((T, FS), BF16),
                pltpu.VMEM((T, FS), BF16),
                pltpu.VMEM((D, FS), BF16),
                pltpu.VMEM((FS, D), BF16),
                pltpu.VMEM((2, 4, SIDE, SIDE, R, Q), F32),
                pltpu.VMEM((2, 4, SIDE, R, Q), F32),
                pltpu.VMEM((2, 4, SIDE, R, Q), F32),
                pltpu.VMEM((SIDE, 4, SIDE, R, Q), F32),
                pltpu.VMEM((2, 2, 6, SIDE, R, Q), F32),
                pltpu.VMEM((2, 2, 6, R, Q), F32),
                pltpu.VMEM((2, R, D), F32),
                pltpu.VMEM((3, 1, D), F32),
                pltpu.VMEM((7, 1, D), F32),
                pltpu.VMEM((2, 256, FS), F32),
                dma((96,)), dma((96,)),
                dma((2, 2, 6)), dma((2, 2, 6)),
                dma((2, 2, 6)), dma((2, 2, 6)),
                dma((2,)), dma((SIDE,)),
                dma((7,)), dma((7,)),
                dma((5,)),
                reg((4,)), reg((4,)), reg((SIDE,)),
            ],
            compiler_params=pltpu.CompilerParams(
                collective_id=0, has_side_effects=True, vmem_limit_bytes=67043328),
        )(X, gamma.reshape(1, D), W1, W2, dY)
        Y, dX, dg, dW1, dW2 = pl.pallas_call(
            _out_kernel,
            out_shape=tuple(jax.ShapeDtypeStruct(v.shape, v.dtype) for v in raw),
            in_specs=[anyspace] * 5,
            out_specs=(anyspace,) * 5,
            scratch_shapes=[pltpu.VMEM(v.shape, v.dtype) for v in raw] + [dma((2, 32))],
        )(*raw)
        return Y, dX, dW1, dW2, dg.reshape(D)

    return jax.shard_map(body, mesh=mesh,
                         in_specs=(rows, P(None), P(None, "tp"), P("tp", None), rows),
                         out_specs=(rows, rows, P("data", "tp"), rows, P("data")),
                         check_vma=False)
```

```python
import math

import jax
import jax.numpy as jnp
from jax import lax
from jax.experimental import pallas as pl
from jax.experimental.pallas import tpu as pltpu
from jax.sharding import PartitionSpec as P

EPS = 1e-6
BF16 = jnp.bfloat16
F32 = jnp.float32
MESH = pl.DeviceIdType.MESH

REL = (0, 1, -1, 2)
IX = {0: 0, 1: 1, -1: 2, 2: 3}
ORDER = (0, 1, -1, 2)
SIDE = 4


def _dot(a, b, ca, cb):
    return lax.dot_general(a, b, (((ca,), (cb,)), ((), ())), preferred_element_type=F32)


def _ln(x):
    mu = jnp.mean(x, axis=-1, keepdims=True)
    xc = x - mu
    var = jnp.mean(xc * xc, axis=-1, keepdims=True)
    rstd = lax.rsqrt(var + EPS)
    return xc * rstd, rstd


def _gelu_and_grad(a):
    c = math.sqrt(2.0 / math.pi)
    a2 = a * a
    t = jnp.tanh(c * (a + 0.044715 * (a2 * a)))
    cdf = 0.5 * (1.0 + t)
    grad = cdf + (0.5 * a * (1.0 - t * t)) * (c + (3.0 * 0.044715 * c) * a2)
    return a * cdf, grad


def _kernel(x_ref, g_ref, w1_hbm, w2_hbm, dy_hbm,
            y_out, dx_out, dg_out, dw1_hbm, dw2_hbm,
            xn, dy, h, da, w1, w2, acc, zbuf, stage, sibr, r1, r2, ysum, gam, gin, dwst,
            ags, agr, p1s, p1r, p2s, p2r, sbs, sbr, gs, gr, lsem, c1, c2, csib):
    me = lax.axis_index("tp")
    core = me % 2
    cx = (me // 2) % SIDE
    cy = me // (2 * SIDE)

    def dev(yy, xx, cc):
        return {"tp": ((yy % SIDE) * SIDE + (xx % SIDE)) * 2 + cc}

    yp, ym, yf = dev(cy + 1, cx, core), dev(cy + SIDE - 1, cx, core), dev(cy + 2, cx, core)
    xp, xm, xf = dev(cy, cx + 1, core), dev(cy, cx + SIDE - 1, core), dev(cy, cx + 2, core)
    sib = dev(cy, cx, 1 - core)

    R = x_ref.shape[0]
    HR = R // 2
    D = x_ref.shape[1]
    FS = w1.shape[1]
    BLK = 2 * SIDE * R
    OWN = SIDE * R
    C = D // 2
    Q = C // 4

    cw1 = pltpu.make_async_copy(w1_hbm, w1, lsem.at[0])
    cw2 = pltpu.make_async_copy(w2_hbm, w2, lsem.at[1])
    cdy = pltpu.make_async_copy(dy_hbm, dy.at[pl.ds(0, R)], lsem.at[2])
    cdy.start()
    cw1.start()
    cw2.start()
    xhat, rstd = _ln(x_ref[...].astype(F32))
    xn[0:R, :] = (xhat * g_ref[...]).astype(BF16)

    bar = pltpu.get_barrier_semaphore()
    for d in (yp, ym, yf, xp, xm, xf, sib):
        pl.semaphore_signal(bar, inc=1, device_id=d, device_id_type=MESH)
    pl.semaphore_wait(bar, 7)

    def remote(src, dst, ss, rs, d):
        return pltpu.make_async_remote_copy(src_ref=src, dst_ref=dst, send_sem=ss, recv_sem=rs, device_id=d, device_id_type=MESH)

    pending = []

    def go(*cs):
        for c in cs:
            c.start()
            pending.append(c)

    def got(*cs):
        for c in cs:
            c.wait_recv()

    class Half:
        def __init__(self, buf, col, first, second, xfirst, base):
            n = [base]

            def at(a, b, half=None):
                dd, ee = (b, a) if xfirst else (a, b)
                o = (IX[dd] * 2 * SIDE + IX[ee]) * R
                if half is None:
                    return buf.at[pl.ds(o, R), pl.ds(col, C)]
                return buf.at[pl.ds(o + half * HR, HR), pl.ds(col, C)]

            def mk(src, dst, d):
                i = n[0]
                n[0] += 1
                return remote(src, dst, ags.at[base // 48], agr.at[i], d)

            (fp, fm), (sp, sm) = first, second
            self.d1 = (mk(at(0, 0), at(-1, 0), fp), mk(at(0, 0), at(1, 0), fm))
            self.d1h = (mk(at(-1, 0, 0), at(2, 0, 0), fp), mk(at(1, 0, 1), at(2, 0, 1), fm))
            self.d2 = {r: (mk(at(r, 0), at(r, -1), sp), mk(at(r, 0), at(r, 1), sm)) for r in REL}
            self.d2h = {r: (mk(at(r, -1, 0), at(r, 2, 0), sp), mk(at(r, 1, 1), at(r, 2, 1), sm)) for r in REL}

        def hop1(self):
            for c, n in zip(self.d1, self.d1h):
                got(c)
                go(n)

        def hop2(self, r):
            for c, n in zip(self.d2[r], self.d2h[r]):
                got(c)
                go(n)

    class Gather:
        def __init__(self, buf, base):
            self.xy = Half(buf, 0, (xp, xm), (yp, ym), True, base)
            self.yx = Half(buf, C, (yp, ym), (xp, xm), False, base + 20)
            self.sb = {r: tuple(remote(buf.at[pl.ds(IX[r] * BLK + o, n)], buf.at[pl.ds(IX[r] * BLK + OWN + o, n)],
                                       ags.at[base // 48], agr.at[base + 40 + 2 * IX[r] + j], sib)
                                for j, (o, n) in enumerate(((0, OWN - R), (OWN - R, R)))) for r in REL}

        def s0(self):
            go(*self.xy.d1, *self.yx.d1, *self.xy.d2[0], *self.yx.d2[0])

        def s1(self):
            self.xy.hop1()
            self.yx.hop1()

        def s1b(self):
            for r in (1, -1):
                go(*self.xy.d2[r], *self.yx.d2[r])

        def s2(self):
            self.xy.hop2(0)
            self.yx.hop2(0)
            go(self.sb[0][0])

        def s3(self):
            got(*self.xy.d1h, *self.yx.d1h)
            go(*self.xy.d2[2], *self.yx.d2[2])

        def s4(self):
            got(*self.yx.d2h[0])
            go(self.sb[0][1])

        def s5(self):
            for r in (1, -1):
                self.xy.hop2(r)
                self.yx.hop2(r)
            go(self.sb[1][0], self.sb[-1][0])

        def s6(self):
            self.xy.hop2(2)
            self.yx.hop2(2)

        def s7(self):
            for r in (1, -1):
                got(*self.yx.d2h[r])
                go(self.sb[r][1])

        def s8(self):
            got(*self.xy.d2h[0], *self.xy.d2h[1], *self.xy.d2h[-1])
            go(self.sb[2][0])
            got(*self.xy.d2h[2], *self.yx.d2h[2])
            go(self.sb[2][1])

    TF = FS // 2

    def keep(dd, f):
        if dd in (0, 1):
            return [[acc.at[1, 2 * f + j, (0, 3)[c] if dd == 0 else (1, 2)[c]] for j in range(2)] for c in range(2)]
        if dd == 2:
            return [[zbuf.at[c, 2 * f + j] for j in range(2)] for c in range(2)]
        return [[dwst.at[c, :, pl.ds(pl.multiple_of(f * TF + j * Q, Q), Q)] for j in range(2)] for c in range(2)]

    def forward_h(dd):
        o = IX[dd] * BLK

        def step(f, _):
            fo = pl.multiple_of(f * TF, TF)
            a = _dot(xn[o:o + BLK, :], w1[:, pl.ds(fo, TF)], 1, 0)
            hv, gv = _gelu_and_grad(a)
            h[o:o + BLK, pl.ds(fo, TF)] = hv.astype(BF16)
            for c, row in enumerate(keep(dd, f)):
                for j, ref in enumerate(row):
                    ref[...] = gv[c * OWN:(c + 1) * OWN, j * Q:(j + 1) * Q].reshape(ref.shape)
            return 0

        lax.fori_loop(0, FS // TF, step, 0)

    def backward_h(dd):
        o = IX[dd] * BLK

        def step(f, _):
            fo = pl.multiple_of(f * TF, TF)
            dh = _dot(dy[o:o + BLK, :], w2[pl.ds(fo, TF), :], 1, 1)
            for c, row in enumerate(keep(dd, f)):
                for j, ref in enumerate(row):
                    co = pl.multiple_of(fo + j * Q, Q)
                    da[o + c * OWN:o + (c + 1) * OWN, pl.ds(co, Q)] = (
                        ref[...].reshape(OWN, Q) * dh[c * OWN:(c + 1) * OWN, j * Q:(j + 1) * Q]).astype(BF16)
            return 0

        lax.fori_loop(0, FS // TF, step, 0)

    ROUND = ((0, 0), (1, 0), (1, 1), (0, 1))
    live = {}
    slots = [None, None]
    count = [0]

    def mblk(k, i):
        s, slot, o = k % 2, count[0] % 2, i * BLK
        back, half = ROUND[k]
        count[0] += 1
        if slots[slot] is not None:
            slots[slot].wait_send()

        def step(n, _):
            co = pl.multiple_of(half * C + n * (2 * Q), 2 * Q)
            if back:
                t = _dot(da[o:o + BLK, :], w1[pl.ds(co, 2 * Q), :], 1, 1)
            else:
                t = _dot(h[o:o + BLK, :], w2[:, pl.ds(co, 2 * Q)], 1, 0)
            for j in range(2):
                acc[s, 2 * n + j, i] = t[:OWN, j * Q:(j + 1) * Q].reshape(SIDE, R, Q)
                stage[slot, 2 * n + j] = t[OWN:, j * Q:(j + 1) * Q].reshape(SIDE, R, Q)
            return 0

        lax.fori_loop(0, 2, step, 0)
        if k > 0:
            pl.semaphore_wait(csib.at[i], 1)
        c = remote(stage.at[slot], sibr.at[i], sbs.at[slot], sbr.at[i], sib)
        c.start()
        slots[slot] = c
        live["sib", k, i] = c

    def add(k, i):
        live.pop(("sib", k, i)).wait_recv()
        for q in range(4):
            acc[k % 2, q, i] = acc[k % 2, q, i] + sibr[i, q]
        if k < 3:
            pl.semaphore_signal(csib.at[i], inc=1, device_id=sib, device_id_type=MESH)

    YR, XR = (yp, ym), (xp, xm)

    def ring_copies(get, buf, ss, rs, ring, cut=0, early=False):
        plus, minus = ring
        src = [(get(0, 2), plus), (get(1, 2), minus), (get(1, 1), plus), (get(0, -1), minus), (get(0, 1), plus), (get(1, -1), minus)]
        out = [[remote(v, buf.at[j], ss, rs.at[j], d)] for j, (v, d) in enumerate(src[:6 - 2 * cut])]
        if early:
            for j in range(4):
                v, d = src[j]
                out[j] = [remote(v.at[pl.ds(o, n)], buf.at[j, pl.ds(o, n)], ss, rs.at[j + 8 * c], d)
                          for c, (o, n) in enumerate(((0, 3), (3, 1)))]
        for j in range(6 - 2 * cut, 6):
            v, d = src[j]
            out.append([remote(v.at[pl.ds(o, 2)], buf.at[j, pl.ds(o, 2)], ss, rs.at[j + 2 * c], d)
                        for c, o in enumerate((2, 0))])
        return out

    def p1_get(k, ab):
        if ab == 0:
            return lambda p, r: acc.at[k % 2, p, IX[r]]
        return lambda p, r: acc.at[k % 2, 2 + p, :, IX[r]]

    def p2_get(k, ab):
        return lambda p, r: zbuf.at[k % 2, 2 * ab + p, IX[r]]

    def begin(k):
        if k >= 2:
            for i in range(4):
                pl.semaphore_wait(c1.at[i], 1)
        s = k % 2
        live["c1", k] = [ring_copies(p1_get(k, ab), r1.at[s, ab], p1s.at[s], p1r.at[s, ab], (YR, XR)[ab], k // 3, ab == 1 and k < 2) for ab in range(2)]

    def send_p1(k, js):
        for j in js:
            for ab in range(2):
                for c in live["c1", k][ab][j]:
                    c.start()

    def e1(k):
        begin(k)
        send_p1(k, range(4))

    def e1_early(k):
        begin(k)
        a, b = live["c1", k]
        for j in range(4):
            b[j][0].start()
        for j in (2, 3):
            a[j][0].start()

    def e1_late(k):
        a, b = live["c1", k]
        for j in (0, 1):
            a[j][0].start()
        for j in range(4):
            b[j][1].start()

    def forward(get, buf, cs, ab):
        for j, p, r in ((0, 0, 1), (1, 1, -1)):
            got(*cs[ab][j])
            v = get(p, r)
            v[...] = v[...] + buf[ab, j]
            for c in cs[ab][4 + j]:
                c.start()

    def final(get, buf, cs, ab):
        for j in (2, 3, 4, 5):
            got(*cs[ab][j])
        return (get(0, 0)[...] + buf[ab, 3] + buf[ab, 4], get(1, 0)[...] + buf[ab, 2] + buf[ab, 5])

    def credit(c):
        for i, d in enumerate((ym, yp, xm, xp)):
            pl.semaphore_signal(c.at[i], inc=1, device_id=d, device_id_type=MESH)

    def drained(key):
        live.pop(key)
        buf, ss = {"c1": (r1, p1s), "c2": (r2, p2s)}[key[0]]
        s = key[1] % 2
        pltpu.make_async_copy(buf.at[s], buf.at[s], ss.at[s]).wait()

    def e2(k, abs_=(0, 1)):
        for ab in abs_:
            forward(p1_get(k, ab), r1.at[k % 2], live["c1", k], ab)

    def e3(k):
        s = k % 2
        if k >= 2:
            drained(("c2", k - 2))
            for i in range(4):
                pl.semaphore_wait(c2.at[i], 1)
        ds = [ring_copies(p2_get(k, ab), r2.at[s, ab], p2s.at[s], p2r.at[s, ab], (XR, YR)[ab]) for ab in range(2)]
        live["c2", k] = ds
        for ab in range(2):
            a, b = final(p1_get(k, ab), r1.at[s], live["c1", k], ab)
            zbuf[s, 2 * ab] = a
            zbuf[s, 2 * ab + 1] = b
            for j in range(4):
                ds[ab][j][0].start()
        if k < 2:
            credit(c1)

    def e3_last(k, c):
        s = k % 2
        if c == 0:
            drained(("c2", k - 2))
            for i in range(4):
                pl.semaphore_wait(c2.at[i], 1)
            live["c2", k] = [ring_copies(p2_get(k, ab), r2.at[s, ab], p2s.at[s], p2r.at[s, ab], (XR, YR)[ab]) for ab in range(2)]
        for ab in range(2):
            cs, get, o = live["c1", k][ab], p1_get(k, ab), pl.ds(2 - 2 * c, 2)
            if c == 0:
                got(*cs[2], *cs[3])
            for p, ja, jb in ((0, 3, 4), (1, 2, 5)):
                got(cs[jb][c])
                zbuf[s, 2 * ab + p, o] = get(p, 0)[o] + r1[s, ab, ja, o] + r1[s, ab, jb, o]
            for j in ((0, 1, 3), (2,))[c]:
                live["c2", k][ab][j][0].start()

    def e4(k):
        for ab in range(2):
            forward(p2_get(k, ab), r2.at[k % 2], live["c2", k], ab)

    def e5(k):
        back, half = ROUND[k]
        for ab in range(2):
            a, b = final(p2_get(k, ab), r2.at[k % 2], live["c2", k], ab)
            o = half * C + 2 * ab * Q
            ysum[back, :, o:o + Q] = a
            ysum[back, :, o + Q:o + 2 * Q] = b
        if k < 2:
            credit(c2)

    TM = dwst.shape[1]
    NT2 = FS // TM * (D // FS)
    NT1 = D // TM

    def dw2_copy(i):
        r = pl.multiple_of((i // 2) * TM, TM)
        c = pl.multiple_of((i % 2) * FS, FS)
        return pltpu.make_async_copy(dwst.at[i % 2], dw2_hbm.at[pl.ds(r, TM), pl.ds(c, FS)], lsem.at[3 + i % 2])

    def dw1_copy(i):
        r = pl.multiple_of(i * TM, TM)
        return pltpu.make_async_copy(dwst.at[i % 2], dw1_hbm.at[pl.ds(r, TM), :], lsem.at[3 + i % 2])

    def dw2_tile(i):
        r = pl.multiple_of((i // 2) * TM, TM)
        c = pl.multiple_of((i % 2) * FS, FS)
        return _dot(h[:, pl.ds(r, TM)], dy[:, pl.ds(c, FS)], 0, 0)

    def dw1_tile(i):
        r = pl.multiple_of(i * TM, TM)
        return _dot(xn[:, pl.ds(r, TM)], da[...], 0, 0)

    done = [0]

    def dw(n):
        i0 = done[0]
        done[0] += n
        copy, tile, lo, total = (dw2_copy, dw2_tile, i0, NT2) if i0 < NT2 else (dw1_copy, dw1_tile, i0 - NT2, NT1)
        hi = lo + n
        assert hi <= total

        def step(i, _):
            @pl.when(i >= 2)
            def _():
                copy(i - 2).wait()
            dwst[i % 2] = tile(i)
            copy(i).start()
            return 0

        lax.fori_loop(lo, hi, step, 0)
        if hi == total:
            copy(total - 2).wait()
            copy(total - 1).wait()

    gx = Gather(xn, 0)
    gy = Gather(dy, 48)

    gx.s0()
    gx.s1()
    gx.s2()
    gx.s1b()
    gx.s3()
    gx.s4()
    cw1.wait()
    got(*gx.sb[0])
    forward_h(0)
    gx.s5()
    cw2.wait()
    mblk(0, 0)
    gx.s6()
    cdy.wait()
    gy.s0()
    gx.s7()
    gx.s8()
    add(0, 0)
    got(*gx.sb[1])
    forward_h(1)
    gy.s1()
    gy.s2()
    gy.s1b()
    mblk(0, 1)
    got(*gx.sb[-1])
    forward_h(-1)
    gy.s3()
    mblk(0, 2)
    add(0, 1)
    gy.s4()
    got(*gx.sb[2])
    forward_h(2)
    gy.s5()
    add(0, 2)
    e1_early(0)
    mblk(0, 3)
    gy.s6()
    got(*gy.sb[0])
    backward_h(0)
    add(0, 3)
    e1_late(0)
    mblk(1, 0)
    gy.s7()
    got(*gy.sb[1])
    backward_h(1)
    add(1, 0)
    mblk(1, 1)
    gy.s8()
    got(*gy.sb[-1])
    backward_h(-1)
    add(1, 1)
    e2(0)
    mblk(1, 2)
    got(*gy.sb[2])
    backward_h(2)
    add(1, 2)
    mblk(1, 3)
    e1_early(1)
    dw(2)
    add(1, 3)
    e1_late(1)
    e3(0)
    drained(("c1", 0))
    mblk(2, 0)
    mblk(2, 1)
    add(2, 0)
    mblk(2, 2)
    add(2, 1)
    mblk(2, 3)
    add(2, 2)
    e2(1)
    dw(2)
    add(2, 3)
    e1(2)
    e4(0)
    dw(2)
    e3(1)
    drained(("c1", 1))
    mblk(3, 0)
    mblk(3, 1)
    add(3, 0)
    mblk(3, 2)
    add(3, 1)
    mblk(3, 3)
    add(3, 2)
    dw(2)
    add(3, 3)
    e2(2)
    e4(1)
    begin(3)
    send_p1(3, (0, 1))
    e5(0)
    dw(4)
    e3(2)
    send_p1(3, (2, 3))
    dw(2)
    e5(1)
    e4(2)
    e2(3)
    dw(2)
    for i, buf in enumerate((xn, dy)):
        all_sent = buf.at[pl.ds(0, 31 * R)]
        pltpu.make_async_copy(all_sent, all_sent, ags.at[i]).wait()
    pending.clear()

    xhat, rstd = _ln(x_ref[...].astype(F32))
    e5(2)
    dxn = ysum[1]
    gam[0] = jnp.sum(dxn * xhat, axis=0, keepdims=True)
    cs = [remote(gam.at[0], gin.at[0], gs.at[0], gr.at[0], sib)]
    cs += [remote(gam.at[1], gin.at[1 + j], gs.at[1 + j], gr.at[1 + j], d) for j, d in enumerate((xp, xm, xf))]
    cs += [remote(gam.at[2], gin.at[4 + j], gs.at[4 + j], gr.at[4 + j], d) for j, d in enumerate((yp, ym, yf))]
    go(cs[0])
    dxhat = dxn * g_ref[...]
    dx = rstd * (dxhat - jnp.mean(dxhat, axis=-1, keepdims=True) - xhat * jnp.mean(dxhat * xhat, axis=-1, keepdims=True))
    dx_out[...] = (dy[0:R, :].astype(F32) + dx).astype(BF16)
    got(cs[0])
    gam[1] = gam[0] + gin[0]
    go(*cs[1:4])
    e3_last(3, 0)
    e3_last(3, 1)
    got(*cs[1:4])
    gam[2] = gam[1] + gin[1] + gin[2] + gin[3]
    go(*cs[4:7])
    e4(3)
    e5(3)
    y_out[...] = (x_ref[...].astype(F32) + ysum[0]).astype(BF16)
    got(*cs[4:7])
    dg_out[...] = gam[2] + gin[4] + gin[5] + gin[6]
    for c in pending + [v for v in slots]:
        c.wait_send()
    for key in (("c1", 2), ("c1", 3), ("c2", 2), ("c2", 3)):
        drained(key)


def _out_kernel(*refs):
    n = (len(refs) - 1) // 3
    src, dst, buf, sem = refs[:n], refs[n:2 * n], refs[2 * n:3 * n], refs[3 * n]
    reads, writes = [], []
    for s, d, b in zip(src, dst, buf):
        m = max(1, s.shape[0] * s.shape[1] * s.dtype.itemsize // 2 ** 20)
        r = s.shape[0] // m
        for i in range(m):
            j = len(reads)
            part = pl.ds(i * r, r)
            reads.append(pltpu.make_async_copy(s.at[part], b.at[part], sem.at[0, j]))
            writes.append(pltpu.make_async_copy(b.at[part], d.at[part], sem.at[1, j]))
    for c in reads:
        c.start()
    for c, w in zip(reads, writes):
        c.wait()
        w.start()
    for w in writes:
        w.wait()


def solution(mesh):
    rows = P(("data", "tp"), None)
    assert mesh.shape["tp"] == 2 * SIDE * SIDE

    def body(X, gamma, W1, W2, dY):
        R, D = X.shape
        FS = W1.shape[1]
        T = R * 2 * SIDE * SIDE
        C = D // 2
        Q = C // 4
        vm = pl.BlockSpec(memory_space=pltpu.VMEM)
        anyspace = pl.BlockSpec(memory_space=pl.ANY)
        dma = pltpu.SemaphoreType.DMA
        reg = pltpu.SemaphoreType.REGULAR
        raw = pl.pallas_call(
            _kernel,
            out_shape=(
                jax.ShapeDtypeStruct((R, D), BF16),
                jax.ShapeDtypeStruct((R, D), BF16),
                jax.ShapeDtypeStruct((1, D), F32),
                jax.ShapeDtypeStruct((D, FS), F32),
                jax.ShapeDtypeStruct((FS, D), F32),
            ),
            in_specs=[vm, vm, anyspace, anyspace, anyspace],
            out_specs=(vm, vm, vm, anyspace, anyspace),
            scratch_shapes=[
                pltpu.VMEM((T, D), BF16),
                pltpu.VMEM((T, D), BF16),
                pltpu.VMEM((T, FS), BF16),
                pltpu.VMEM((T, FS), BF16),
                pltpu.VMEM((D, FS), BF16),
                pltpu.VMEM((FS, D), BF16),
                pltpu.VMEM((2, 4, SIDE, SIDE, R, Q), F32),
                pltpu.VMEM((2, 4, SIDE, R, Q), F32),
                pltpu.VMEM((2, 4, SIDE, R, Q), F32),
                pltpu.VMEM((SIDE, 4, SIDE, R, Q), F32),
                pltpu.VMEM((2, 2, 6, SIDE, R, Q), F32),
                pltpu.VMEM((2, 2, 6, R, Q), F32),
                pltpu.VMEM((2, R, D), F32),
                pltpu.VMEM((3, 1, D), F32),
                pltpu.VMEM((7, 1, D), F32),
                pltpu.VMEM((2, 256, FS), F32),
                dma((2,)), dma((96,)),
                dma((2,)), dma((2, 2, 12)),
                dma((2,)), dma((2, 2, 6)),
                dma((2,)), dma((SIDE,)),
                dma((7,)), dma((7,)),
                dma((5,)),
                reg((4,)), reg((4,)), reg((SIDE,)),
            ],
            compiler_params=pltpu.CompilerParams(
                collective_id=0, has_side_effects=True, vmem_limit_bytes=67043328),
        )(X, gamma.reshape(1, D), W1, W2, dY)
        Y, dX, dg, dW1, dW2 = pl.pallas_call(
            _out_kernel,
            out_shape=tuple(jax.ShapeDtypeStruct(v.shape, v.dtype) for v in raw),
            in_specs=[anyspace] * 5,
            out_specs=(anyspace,) * 5,
            scratch_shapes=[pltpu.VMEM(v.shape, v.dtype) for v in raw] + [dma((2, 32))],
        )(*raw)
        return Y, dX, dW1, dW2, dg.reshape(D)

    return jax.shard_map(body, mesh=mesh,
                         in_specs=(rows, P(None), P(None, "tp"), P("tp", None), rows),
                         out_specs=(rows, rows, P("data", "tp"), rows, P("data")),
                         check_vma=False)
```

```python
import math

import jax
import jax.numpy as jnp
from jax import lax
from jax.experimental import pallas as pl
from jax.experimental.pallas import tpu as pltpu
from jax.sharding import PartitionSpec as P

EPS = 1e-6
BF16 = jnp.bfloat16
F32 = jnp.float32
MESH = pl.DeviceIdType.MESH

REL = (0, 1, -1, 2)
IX = {0: 0, 1: 1, -1: 2, 2: 3}
ORDER = (0, 1, -1, 2)
SIDE = 4


def _dot(a, b, ca, cb):
    return lax.dot_general(a, b, (((ca,), (cb,)), ((), ())), preferred_element_type=F32)


def _ln(x):
    mu = jnp.mean(x, axis=-1, keepdims=True)
    xc = x - mu
    var = jnp.mean(xc * xc, axis=-1, keepdims=True)
    rstd = lax.rsqrt(var + EPS)
    return xc * rstd, rstd


def _gelu_and_grad(a):
    c = math.sqrt(2.0 / math.pi)
    a2 = a * a
    t = jnp.tanh(c * (a + 0.044715 * (a2 * a)))
    cdf = 0.5 * (1.0 + t)
    grad = cdf + (0.5 * a * (1.0 - t * t)) * (c + (3.0 * 0.044715 * c) * a2)
    return a * cdf, grad


def _kernel(x_ref, g_ref, w1_hbm, w2_hbm, dy_hbm,
            y_out, dx_out, dg_out, acc, sibr, dw2_hbm,
            xn, dy, h, da, w1, w2, zbuf, stage, r1, r2, ysum, gam, gin, dwst,
            ags, agr, p1s, p1r, p2s, p2r, sbs, sbr, gs, gr, lsem, c1, c2, csib):
    me = lax.axis_index("tp")
    core = me % 2
    cx = (me // 2) % SIDE
    cy = me // (2 * SIDE)

    def dev(yy, xx, cc):
        return {"tp": ((yy % SIDE) * SIDE + (xx % SIDE)) * 2 + cc}

    yp, ym, yf = dev(cy + 1, cx, core), dev(cy + SIDE - 1, cx, core), dev(cy + 2, cx, core)
    xp, xm, xf = dev(cy, cx + 1, core), dev(cy, cx + SIDE - 1, core), dev(cy, cx + 2, core)
    sib = dev(cy, cx, 1 - core)

    R = x_ref.shape[0]
    HR = R // 2
    D = x_ref.shape[1]
    FS = w1.shape[1]
    BLK = 2 * SIDE * R
    OWN = SIDE * R
    C = D // 2
    Q = C // 4

    cw1 = pltpu.make_async_copy(w1_hbm, w1, lsem.at[0])
    cw2 = pltpu.make_async_copy(w2_hbm, w2, lsem.at[1])
    cdy = pltpu.make_async_copy(dy_hbm, dy.at[pl.ds(0, R)], lsem.at[2])
    cdy.start()
    cw1.start()
    cw2.start()
    xhat, rstd = _ln(x_ref[...].astype(F32))
    xn[0:R, :] = (xhat * g_ref[...]).astype(BF16)

    bar = pltpu.get_barrier_semaphore()
    for d in (yp, ym, yf, xp, xm, xf, sib):
        pl.semaphore_signal(bar, inc=1, device_id=d, device_id_type=MESH)
    pl.semaphore_wait(bar, 7)

    def remote(src, dst, ss, rs, d):
        return pltpu.make_async_remote_copy(src_ref=src, dst_ref=dst, send_sem=ss, recv_sem=rs, device_id=d, device_id_type=MESH)

    pending = []

    def go(*cs):
        for c in cs:
            c.start()
            pending.append(c)

    def got(*cs):
        for c in cs:
            c.wait_recv()

    class Half:
        def __init__(self, buf, col, first, second, xfirst, base):
            n = [base]

            def at(a, b, half=None):
                dd, ee = (b, a) if xfirst else (a, b)
                o = (IX[dd] * 2 * SIDE + IX[ee]) * R
                if half is None:
                    return buf.at[pl.ds(o, R), pl.ds(col, C)]
                return buf.at[pl.ds(o + half * HR, HR), pl.ds(col, C)]

            def mk(src, dst, d):
                i = n[0]
                n[0] += 1
                return remote(src, dst, ags.at[base // 48], agr.at[i], d)

            (fp, fm), (sp, sm) = first, second
            self.d1 = (mk(at(0, 0), at(-1, 0), fp), mk(at(0, 0), at(1, 0), fm))
            self.d1h = (mk(at(-1, 0, 0), at(2, 0, 0), fp), mk(at(1, 0, 1), at(2, 0, 1), fm))
            self.d2 = {r: (mk(at(r, 0), at(r, -1), sp), mk(at(r, 0), at(r, 1), sm)) for r in REL}
            self.d2h = {r: (mk(at(r, -1, 0), at(r, 2, 0), sp), mk(at(r, 1, 1), at(r, 2, 1), sm)) for r in REL}

        def hop1(self):
            for c, n in zip(self.d1, self.d1h):
                got(c)
                go(n)

        def hop2(self, r):
            for c, n in zip(self.d2[r], self.d2h[r]):
                got(c)
                go(n)

    class Gather:
        def __init__(self, buf, base):
            self.xy = Half(buf, 0, (xp, xm), (yp, ym), True, base)
            self.yx = Half(buf, C, (yp, ym), (xp, xm), False, base + 20)
            self.sb = {r: tuple(remote(buf.at[pl.ds(IX[r] * BLK + o, n)], buf.at[pl.ds(IX[r] * BLK + OWN + o, n)],
                                       ags.at[base // 48], agr.at[base + 40 + 2 * IX[r] + j], sib)
                                for j, (o, n) in enumerate(((0, OWN - R), (OWN - R, R)))) for r in REL}

        def s0(self):
            go(*self.xy.d1, *self.yx.d1, *self.xy.d2[0], *self.yx.d2[0])

        def s1(self):
            self.xy.hop1()
            self.yx.hop1()

        def s1b(self):
            for r in (1, -1):
                go(*self.xy.d2[r], *self.yx.d2[r])

        def s2(self):
            self.xy.hop2(0)
            self.yx.hop2(0)
            go(self.sb[0][0])

        def s3(self):
            got(*self.xy.d1h, *self.yx.d1h)
            go(*self.xy.d2[2], *self.yx.d2[2])

        def s4(self):
            got(*self.yx.d2h[0])
            go(self.sb[0][1])

        def s5(self):
            for r in (1, -1):
                self.xy.hop2(r)
                self.yx.hop2(r)
            go(self.sb[1][0], self.sb[-1][0])

        def s6(self):
            self.xy.hop2(2)
            self.yx.hop2(2)

        def s7(self):
            for r in (1, -1):
                got(*self.yx.d2h[r])
                go(self.sb[r][1])

        def s8(self):
            got(*self.xy.d2h[0], *self.xy.d2h[1], *self.xy.d2h[-1])
            go(self.sb[2][0])
            got(*self.xy.d2h[2], *self.yx.d2h[2])
            go(self.sb[2][1])

    TF = FS // 2

    def keep(dd, f):
        if dd in (0, 1):
            return [[acc.at[1, 2 * f + j, (0, 3)[c] if dd == 0 else (1, 2)[c]] for j in range(2)] for c in range(2)]
        if dd == 2:
            return [[zbuf.at[c, 2 * f + j] for j in range(2)] for c in range(2)]
        return [[dwst.at[c, :, pl.ds(pl.multiple_of(f * TF + j * Q, Q), Q)] for j in range(2)] for c in range(2)]

    def forward_h(dd):
        o = IX[dd] * BLK

        def step(f, _):
            fo = pl.multiple_of(f * TF, TF)
            a = _dot(xn[o:o + BLK, :], w1[:, pl.ds(fo, TF)], 1, 0)
            hv, gv = _gelu_and_grad(a)
            h[o:o + BLK, pl.ds(fo, TF)] = hv.astype(BF16)
            for c, row in enumerate(keep(dd, f)):
                for j, ref in enumerate(row):
                    ref[...] = gv[c * OWN:(c + 1) * OWN, j * Q:(j + 1) * Q].reshape(ref.shape)
            return 0

        lax.fori_loop(0, FS // TF, step, 0)

    def backward_h(dd):
        o = IX[dd] * BLK

        def step(f, _):
            fo = pl.multiple_of(f * TF, TF)
            dh = _dot(dy[o:o + BLK, :], w2[pl.ds(fo, TF), :], 1, 1)
            for c, row in enumerate(keep(dd, f)):
                for j, ref in enumerate(row):
                    co = pl.multiple_of(fo + j * Q, Q)
                    da[o + c * OWN:o + (c + 1) * OWN, pl.ds(co, Q)] = (
                        ref[...].reshape(OWN, Q) * dh[c * OWN:(c + 1) * OWN, j * Q:(j + 1) * Q]).astype(BF16)
            return 0

        lax.fori_loop(0, FS // TF, step, 0)

    ROUND = ((0, 0), (1, 0), (1, 1), (0, 1))
    live = {}
    slots = [None, None]
    count = [0]

    def mblk(k, i):
        s, slot, o = k % 2, count[0] % 2, i * BLK
        back, half = ROUND[k]
        count[0] += 1
        if slots[slot] is not None:
            slots[slot].wait_send()

        def step(n, _):
            co = pl.multiple_of(half * C + n * (2 * Q), 2 * Q)
            if back:
                t = _dot(da[o:o + BLK, :], w1[pl.ds(co, 2 * Q), :], 1, 1)
            else:
                t = _dot(h[o:o + BLK, :], w2[:, pl.ds(co, 2 * Q)], 1, 0)
            for j in range(2):
                acc[s, 2 * n + j, i] = t[:OWN, j * Q:(j + 1) * Q].reshape(SIDE, R, Q)
                stage[slot, 2 * n + j] = t[OWN:, j * Q:(j + 1) * Q].reshape(SIDE, R, Q)
            return 0

        lax.fori_loop(0, 2, step, 0)
        if k > 0:
            pl.semaphore_wait(csib.at[i], 1)
        c = remote(stage.at[slot], sibr.at[i], sbs.at[slot], sbr.at[i], sib)
        c.start()
        slots[slot] = c
        live["sib", k, i] = c

    def add(k, i):
        live.pop(("sib", k, i)).wait_recv()
        for q in range(4):
            acc[k % 2, q, i] = acc[k % 2, q, i] + sibr[i, q]
        if k < 3:
            pl.semaphore_signal(csib.at[i], inc=1, device_id=sib, device_id_type=MESH)

    YR, XR = (yp, ym), (xp, xm)

    def ring_copies(get, buf, ss, rs, ring, cut=0, early=False):
        plus, minus = ring
        src = [(get(0, 2), plus), (get(1, 2), minus), (get(1, 1), plus), (get(0, -1), minus), (get(0, 1), plus), (get(1, -1), minus)]
        out = [[remote(v, buf.at[j], ss, rs.at[j], d)] for j, (v, d) in enumerate(src[:6 - 2 * cut])]
        if early:
            for j in range(4):
                v, d = src[j]
                out[j] = [remote(v.at[pl.ds(o, n)], buf.at[j, pl.ds(o, n)], ss, rs.at[j + 8 * c], d)
                          for c, (o, n) in enumerate(((0, 3), (3, 1)))]
        for j in range(6 - 2 * cut, 6):
            v, d = src[j]
            out.append([remote(v.at[pl.ds(o, 2)], buf.at[j, pl.ds(o, 2)], ss, rs.at[j + 2 * c], d)
                        for c, o in enumerate((2, 0))])
        return out

    def p1_get(k, ab):
        if ab == 0:
            return lambda p, r: acc.at[k % 2, p, IX[r]]
        return lambda p, r: acc.at[k % 2, 2 + p, :, IX[r]]

    def p2_get(k, ab):
        return lambda p, r: zbuf.at[k % 2, 2 * ab + p, IX[r]]

    def begin(k):
        if k >= 2:
            for i in range(4):
                pl.semaphore_wait(c1.at[i], 1)
        s = k % 2
        live["c1", k] = [ring_copies(p1_get(k, ab), r1.at[s, ab], p1s.at[s], p1r.at[s, ab], (YR, XR)[ab], k // 3, ab == 1 and k < 2) for ab in range(2)]

    def send_p1(k, js):
        for j in js:
            for ab in range(2):
                for c in live["c1", k][ab][j]:
                    c.start()

    def e1(k):
        begin(k)
        send_p1(k, range(4))

    def e1_early(k):
        begin(k)
        a, b = live["c1", k]
        for j in range(4):
            b[j][0].start()
        for j in (2, 3):
            a[j][0].start()

    def e1_late(k):
        a, b = live["c1", k]
        for j in (0, 1):
            a[j][0].start()
        for j in range(4):
            b[j][1].start()

    def forward(get, buf, cs, ab):
        for j, p, r in ((0, 0, 1), (1, 1, -1)):
            got(*cs[ab][j])
            v = get(p, r)
            v[...] = v[...] + buf[ab, j]
            for c in cs[ab][4 + j]:
                c.start()

    def final(get, buf, cs, ab):
        for j in (2, 3, 4, 5):
            got(*cs[ab][j])
        return (get(0, 0)[...] + buf[ab, 3] + buf[ab, 4], get(1, 0)[...] + buf[ab, 2] + buf[ab, 5])

    def credit(c):
        for i, d in enumerate((ym, yp, xm, xp)):
            pl.semaphore_signal(c.at[i], inc=1, device_id=d, device_id_type=MESH)

    def drained(key):
        live.pop(key)
        buf, ss = {"c1": (r1, p1s), "c2": (r2, p2s)}[key[0]]
        s = key[1] % 2
        pltpu.make_async_copy(buf.at[s], buf.at[s], ss.at[s]).wait()

    def e2(k, abs_=(0, 1)):
        for ab in abs_:
            forward(p1_get(k, ab), r1.at[k % 2], live["c1", k], ab)

    def e3(k):
        s = k % 2
        if k >= 2:
            drained(("c2", k - 2))
            for i in range(4):
                pl.semaphore_wait(c2.at[i], 1)
        ds = [ring_copies(p2_get(k, ab), r2.at[s, ab], p2s.at[s], p2r.at[s, ab], (XR, YR)[ab]) for ab in range(2)]
        live["c2", k] = ds
        for ab in range(2):
            a, b = final(p1_get(k, ab), r1.at[s], live["c1", k], ab)
            zbuf[s, 2 * ab] = a
            zbuf[s, 2 * ab + 1] = b
            for j in range(4):
                ds[ab][j][0].start()
        if k < 2:
            credit(c1)

    def e3_last(k, c):
        s = k % 2
        if c == 0:
            drained(("c2", k - 2))
            for i in range(4):
                pl.semaphore_wait(c2.at[i], 1)
            live["c2", k] = [ring_copies(p2_get(k, ab), r2.at[s, ab], p2s.at[s], p2r.at[s, ab], (XR, YR)[ab]) for ab in range(2)]
        for ab in range(2):
            cs, get, o = live["c1", k][ab], p1_get(k, ab), pl.ds(2 - 2 * c, 2)
            if c == 0:
                got(*cs[2], *cs[3])
            for p, ja, jb in ((0, 3, 4), (1, 2, 5)):
                got(cs[jb][c])
                zbuf[s, 2 * ab + p, o] = get(p, 0)[o] + r1[s, ab, ja, o] + r1[s, ab, jb, o]
            for j in ((0, 1, 3), (2,))[c]:
                live["c2", k][ab][j][0].start()

    def e4(k):
        for ab in range(2):
            forward(p2_get(k, ab), r2.at[k % 2], live["c2", k], ab)

    def e5(k):
        back, half = ROUND[k]
        for ab in range(2):
            a, b = final(p2_get(k, ab), r2.at[k % 2], live["c2", k], ab)
            o = half * C + 2 * ab * Q
            ysum[back, :, o:o + Q] = a
            ysum[back, :, o + Q:o + 2 * Q] = b
        if k < 2:
            credit(c2)

    TM = dwst.shape[1]
    NT2 = FS // TM * (D // FS)
    NT1 = D // TM

    def dw2_copy(i):
        r = pl.multiple_of((i // 2) * TM, TM)
        c = pl.multiple_of((i % 2) * FS, FS)
        return pltpu.make_async_copy(dwst.at[i % 2], dw2_hbm.at[pl.ds(r, TM), pl.ds(c, FS)], lsem.at[3 + i % 2])

    def dw2_tile(i):
        r = pl.multiple_of((i // 2) * TM, TM)
        c = pl.multiple_of((i % 2) * FS, FS)
        return _dot(h[:, pl.ds(r, TM)], dy[:, pl.ds(c, FS)], 0, 0)

    def dw1_tile(i):
        r = pl.multiple_of(i * TM, TM)
        return _dot(xn[:, pl.ds(r, TM)], da[...], 0, 0)

    done = [0]

    def dw(n):
        i0 = done[0]
        done[0] += n
        lo, total = (i0, NT2) if i0 < NT2 else (i0 - NT2, NT1)
        hi = lo + n
        assert hi <= total

        def step2(i, _):
            @pl.when(i >= 2)
            def _():
                dw2_copy(i - 2).wait()
            dwst[i % 2] = dw2_tile(i)
            dw2_copy(i).start()
            return 0

        def step1(i, _):
            t = dw1_tile(i)
            for q in range(4):
                v = t[:, q * Q:(q + 1) * Q].reshape(SIDE, R, Q)
                if hi <= SIDE:
                    sibr[i, q] = v
                else:
                    acc[0, q, i - SIDE] = v
            return 0

        lax.fori_loop(lo, hi, step2 if i0 < NT2 else step1, 0)
        if i0 < NT2 and hi == total:
            dw2_copy(total - 2).wait()
            dw2_copy(total - 1).wait()

    gx = Gather(xn, 0)
    gy = Gather(dy, 48)

    gx.s0()
    gx.s1()
    gx.s2()
    gx.s1b()
    gx.s3()
    gx.s4()
    cw1.wait()
    got(*gx.sb[0])
    forward_h(0)
    gx.s5()
    cw2.wait()
    mblk(0, 0)
    gx.s6()
    cdy.wait()
    gy.s0()
    gx.s7()
    gx.s8()
    add(0, 0)
    got(*gx.sb[1])
    forward_h(1)
    gy.s1()
    gy.s2()
    gy.s1b()
    mblk(0, 1)
    got(*gx.sb[-1])
    forward_h(-1)
    gy.s3()
    mblk(0, 2)
    add(0, 1)
    gy.s4()
    got(*gx.sb[2])
    forward_h(2)
    gy.s5()
    add(0, 2)
    e1_early(0)
    mblk(0, 3)
    gy.s6()
    got(*gy.sb[0])
    backward_h(0)
    add(0, 3)
    e1_late(0)
    mblk(1, 0)
    gy.s7()
    got(*gy.sb[1])
    backward_h(1)
    add(1, 0)
    mblk(1, 1)
    gy.s8()
    got(*gy.sb[-1])
    backward_h(-1)
    add(1, 1)
    e2(0)
    mblk(1, 2)
    got(*gy.sb[2])
    backward_h(2)
    add(1, 2)
    mblk(1, 3)
    e1_early(1)
    dw(2)
    add(1, 3)
    e1_late(1)
    e3(0)
    drained(("c1", 0))
    mblk(2, 0)
    mblk(2, 1)
    add(2, 0)
    mblk(2, 2)
    add(2, 1)
    mblk(2, 3)
    add(2, 2)
    e2(1)
    dw(2)
    add(2, 3)
    e1(2)
    e4(0)
    dw(2)
    e3(1)
    drained(("c1", 1))
    mblk(3, 0)
    mblk(3, 1)
    add(3, 0)
    mblk(3, 2)
    add(3, 1)
    mblk(3, 3)
    add(3, 2)
    dw(2)
    add(3, 3)
    e2(2)
    e4(1)
    begin(3)
    send_p1(3, (0, 1))
    e5(0)
    dw(4)
    e3(2)
    send_p1(3, (2, 3))
    drained(("c1", 2))
    dw(2)
    e5(1)
    e4(2)
    e2(3)
    dw(2)
    for i, buf in enumerate((xn, dy)):
        all_sent = buf.at[pl.ds(0, 31 * R)]
        pltpu.make_async_copy(all_sent, all_sent, ags.at[i]).wait()
    pending.clear()

    xhat, rstd = _ln(x_ref[...].astype(F32))
    e5(2)
    dxn = ysum[1]
    gam[0] = jnp.sum(dxn * xhat, axis=0, keepdims=True)
    cs = [remote(gam.at[0], gin.at[0], gs.at[0], gr.at[0], sib)]
    cs += [remote(gam.at[1], gin.at[1 + j], gs.at[1 + j], gr.at[1 + j], d) for j, d in enumerate((xp, xm, xf))]
    cs += [remote(gam.at[2], gin.at[4 + j], gs.at[4 + j], gr.at[4 + j], d) for j, d in enumerate((yp, ym, yf))]
    go(cs[0])
    dxhat = dxn * g_ref[...]
    dx = rstd * (dxhat - jnp.mean(dxhat, axis=-1, keepdims=True) - xhat * jnp.mean(dxhat * xhat, axis=-1, keepdims=True))
    dx_out[...] = (dy[0:R, :].astype(F32) + dx).astype(BF16)
    got(cs[0])
    gam[1] = gam[0] + gin[0]
    go(*cs[1:4])
    e3_last(3, 0)
    e3_last(3, 1)
    got(*cs[1:4])
    gam[2] = gam[1] + gin[1] + gin[2] + gin[3]
    go(*cs[4:7])
    e4(3)
    e5(3)
    y_out[...] = (x_ref[...].astype(F32) + ysum[0]).astype(BF16)
    got(*cs[4:7])
    dg_out[...] = gam[2] + gin[4] + gin[5] + gin[6]
    for c in pending + [v for v in slots]:
        c.wait_send()
    for key in (("c1", 3), ("c2", 2), ("c2", 3)):
        drained(key)


def _out_kernel(y, dx, dg, acc, sibr, dw2, y_out, dx_out, dg_out, dw1_out, dw2_out, by, bdx, bdg, bdw2, sem, one):
    _, P4, _, S4, R, Q = acc.shape
    reads, writes = [], []
    for s, d, b in ((dw2, dw2_out, bdw2), (y, y_out, by), (dx, dx_out, bdx), (dg, dg_out, bdg)):
        m = max(1, s.shape[0] * s.shape[1] * s.dtype.itemsize // 2 ** 20)
        r = s.shape[0] // m
        for i in range(m):
            j = len(reads)
            part = pl.ds(i * r, r)
            reads.append(pltpu.make_async_copy(s.at[part], b.at[part], sem.at[0, j]))
            writes.append(pltpu.make_async_copy(b.at[part], d.at[part], sem.at[1, j]))
    for c in reads:
        c.start()
    for t in range(2 * S4):
        for q in range(P4):
            src = sibr.at[t, q] if t < S4 else acc.at[0, q, t - S4]
            pltpu.make_async_copy(src, dw1_out.at[pl.ds(t * S4, S4), :, pl.ds(q * Q, Q)], one.at[0]).start()
    for c, w in zip(reads, writes):
        c.wait()
        w.start()
    for w in writes:
        w.wait()
    pltpu.make_async_copy(dw1_out, dw1_out, one.at[0]).wait()


def solution(mesh):
    rows = P(("data", "tp"), None)
    assert mesh.shape["tp"] == 2 * SIDE * SIDE

    def body(X, gamma, W1, W2, dY):
        R, D = X.shape
        FS = W1.shape[1]
        T = R * 2 * SIDE * SIDE
        C = D // 2
        Q = C // 4
        vm = pl.BlockSpec(memory_space=pltpu.VMEM)
        anyspace = pl.BlockSpec(memory_space=pl.ANY)
        dma = pltpu.SemaphoreType.DMA
        reg = pltpu.SemaphoreType.REGULAR
        raw = pl.pallas_call(
            _kernel,
            out_shape=(
                jax.ShapeDtypeStruct((R, D), BF16),
                jax.ShapeDtypeStruct((R, D), BF16),
                jax.ShapeDtypeStruct((1, D), F32),
                pltpu.VMEM((2, 4, SIDE, SIDE, R, Q), F32),
                pltpu.VMEM((SIDE, 4, SIDE, R, Q), F32),
                jax.ShapeDtypeStruct((FS, D), F32),
            ),
            in_specs=[vm, vm, anyspace, anyspace, anyspace],
            out_specs=(vm, vm, vm, vm, vm, anyspace),
            scratch_shapes=[
                pltpu.VMEM((T, D), BF16),
                pltpu.VMEM((T, D), BF16),
                pltpu.VMEM((T, FS), BF16),
                pltpu.VMEM((T, FS), BF16),
                pltpu.VMEM((D, FS), BF16),
                pltpu.VMEM((FS, D), BF16),
                pltpu.VMEM((2, 4, SIDE, R, Q), F32),
                pltpu.VMEM((2, 4, SIDE, R, Q), F32),
                pltpu.VMEM((2, 2, 6, SIDE, R, Q), F32),
                pltpu.VMEM((2, 2, 6, R, Q), F32),
                pltpu.VMEM((2, R, D), F32),
                pltpu.VMEM((3, 1, D), F32),
                pltpu.VMEM((7, 1, D), F32),
                pltpu.VMEM((2, 256, FS), F32),
                dma((2,)), dma((96,)),
                dma((2,)), dma((2, 2, 12)),
                dma((2,)), dma((2, 2, 6)),
                dma((2,)), dma((SIDE,)),
                dma((7,)), dma((7,)),
                dma((5,)),
                reg((4,)), reg((4,)), reg((SIDE,)),
            ],
            compiler_params=pltpu.CompilerParams(
                collective_id=0, has_side_effects=True, vmem_limit_bytes=67043328 - 12 * 2 ** 20 - 2 ** 17),
        )(X, gamma.reshape(1, D), W1, W2, dY)
        Y, dX, dg, acc, sibr, dW2 = raw
        acc = pltpu.with_memory_space_constraint(acc, pltpu.VMEM)
        sibr = pltpu.with_memory_space_constraint(sibr, pltpu.VMEM)
        Y, dX, dg, dW2 = (pltpu.with_memory_space_constraint(v, pltpu.HBM) for v in (Y, dX, dg, dW2))
        Y, dX, dg, dW1, dW2 = pl.pallas_call(
            _out_kernel,
            out_shape=(
                jax.ShapeDtypeStruct((R, D), BF16),
                jax.ShapeDtypeStruct((R, D), BF16),
                jax.ShapeDtypeStruct((1, D), F32),
                jax.ShapeDtypeStruct((D // R, R, FS), F32),
                jax.ShapeDtypeStruct((FS, D), F32),
            ),
            in_specs=[anyspace, anyspace, anyspace, vm, vm, anyspace],
            out_specs=(anyspace,) * 5,
            scratch_shapes=[pltpu.VMEM((R, D), BF16), pltpu.VMEM((R, D), BF16), pltpu.VMEM((1, D), F32),
                            pltpu.VMEM((FS, D), F32), dma((2, 16)), dma((1,))],
            compiler_params=pltpu.CompilerParams(vmem_limit_bytes=67043328 - 12 * 2 ** 20 - 2 ** 17),
        )(Y, dX, dg, acc, sibr, dW2)
        return Y, dX, dW1.reshape(D, FS), dW2, dg.reshape(D)

    return jax.shard_map(body, mesh=mesh,
                         in_specs=(rows, P(None), P(None, "tp"), P("tp", None), rows),
                         out_specs=(rows, rows, P("data", "tp"), rows, P("data")),
                         check_vma=False)
```

```python
import math

import jax
import jax.numpy as jnp
from jax import lax
from jax.experimental import pallas as pl
from jax.experimental.pallas import tpu as pltpu
from jax.sharding import PartitionSpec as P

EPS = 1e-6
BF16 = jnp.bfloat16
F32 = jnp.float32
MESH = pl.DeviceIdType.MESH

REL = (0, 1, -1, 2)
IX = {0: 0, 1: 1, -1: 2, 2: 3}
ORDER = (0, 1, -1, 2)
SIDE = 4


def _dot(a, b, ca, cb):
    return lax.dot_general(a, b, (((ca,), (cb,)), ((), ())), preferred_element_type=F32)


def _ln(x):
    mu = jnp.mean(x, axis=-1, keepdims=True)
    xc = x - mu
    var = jnp.mean(xc * xc, axis=-1, keepdims=True)
    rstd = lax.rsqrt(var + EPS)
    return xc * rstd, rstd


def _gelu_and_grad(a):
    c = math.sqrt(2.0 / math.pi)
    a2 = a * a
    t = jnp.tanh(c * (a + 0.044715 * (a2 * a)))
    cdf = 0.5 * (1.0 + t)
    grad = cdf + (0.5 * a * (1.0 - t * t)) * (c + (3.0 * 0.044715 * c) * a2)
    return a * cdf, grad


def _kernel(x_ref, g_ref, w1_hbm, w2_hbm, dy_hbm,
            y_out, dx_out, dg_out, acc, sibr, dwst, dw2_hbm,
            xn, dy, h, da, w1, w2, zbuf, stage, r1, r2, ysum, gam, gin,
            ags, agr, p1s, p1r, p2s, p2r, sbs, sbr, gs, gr, lsem, c1, c2, csib):
    me = lax.axis_index("tp")
    core = me % 2
    cx = (me // 2) % SIDE
    cy = me // (2 * SIDE)

    def dev(yy, xx, cc):
        return {"tp": ((yy % SIDE) * SIDE + (xx % SIDE)) * 2 + cc}

    yp, ym, yf = dev(cy + 1, cx, core), dev(cy + SIDE - 1, cx, core), dev(cy + 2, cx, core)
    xp, xm, xf = dev(cy, cx + 1, core), dev(cy, cx + SIDE - 1, core), dev(cy, cx + 2, core)
    sib = dev(cy, cx, 1 - core)

    R = x_ref.shape[0]
    HR = R // 2
    D = x_ref.shape[1]
    FS = w1.shape[1]
    BLK = 2 * SIDE * R
    OWN = SIDE * R
    C = D // 2
    Q = C // 4

    cw1 = pltpu.make_async_copy(w1_hbm, w1, lsem.at[0])
    cw2 = pltpu.make_async_copy(w2_hbm, w2, lsem.at[1])
    cdy = pltpu.make_async_copy(dy_hbm, dy.at[pl.ds(0, R)], lsem.at[2])
    cdy.start()
    cw1.start()
    cw2.start()
    xhat, rstd = _ln(x_ref[...].astype(F32))
    xn[0:R, :] = (xhat * g_ref[...]).astype(BF16)

    bar = pltpu.get_barrier_semaphore()
    for d in (yp, ym, yf, xp, xm, xf, sib):
        pl.semaphore_signal(bar, inc=1, device_id=d, device_id_type=MESH)
    pl.semaphore_wait(bar, 7)

    def remote(src, dst, ss, rs, d):
        return pltpu.make_async_remote_copy(src_ref=src, dst_ref=dst, send_sem=ss, recv_sem=rs, device_id=d, device_id_type=MESH)

    pending = []

    def go(*cs):
        for c in cs:
            c.start()
            pending.append(c)

    def got(*cs):
        for c in cs:
            c.wait_recv()

    class Half:
        def __init__(self, buf, col, first, second, xfirst, base):
            n = [base]

            def at(a, b, half=None):
                dd, ee = (b, a) if xfirst else (a, b)
                o = (IX[dd] * 2 * SIDE + IX[ee]) * R
                if half is None:
                    return buf.at[pl.ds(o, R), pl.ds(col, C)]
                return buf.at[pl.ds(o + half * HR, HR), pl.ds(col, C)]

            def mk(src, dst, d):
                i = n[0]
                n[0] += 1
                return remote(src, dst, ags.at[base // 48], agr.at[i], d)

            (fp, fm), (sp, sm) = first, second
            self.d1 = (mk(at(0, 0), at(-1, 0), fp), mk(at(0, 0), at(1, 0), fm))
            self.d1h = (mk(at(-1, 0, 0), at(2, 0, 0), fp), mk(at(1, 0, 1), at(2, 0, 1), fm))
            self.d2 = {r: (mk(at(r, 0), at(r, -1), sp), mk(at(r, 0), at(r, 1), sm)) for r in REL}
            self.d2h = {r: (mk(at(r, -1, 0), at(r, 2, 0), sp), mk(at(r, 1, 1), at(r, 2, 1), sm)) for r in REL}

        def hop1(self):
            for c, n in zip(self.d1, self.d1h):
                got(c)
                go(n)

        def hop2(self, r):
            for c, n in zip(self.d2[r], self.d2h[r]):
                got(c)
                go(n)

    class Gather:
        def __init__(self, buf, base):
            self.xy = Half(buf, 0, (xp, xm), (yp, ym), True, base)
            self.yx = Half(buf, C, (yp, ym), (xp, xm), False, base + 20)
            self.sb = {r: tuple(remote(buf.at[pl.ds(IX[r] * BLK + o, n)], buf.at[pl.ds(IX[r] * BLK + OWN + o, n)],
                                       ags.at[base // 48], agr.at[base + 40 + 2 * IX[r] + j], sib)
                                for j, (o, n) in enumerate(((0, OWN - R), (OWN - R, R)))) for r in REL}

        def s0(self):
            go(*self.xy.d1, *self.yx.d1, *self.xy.d2[0], *self.yx.d2[0])

        def s1(self):
            self.xy.hop1()
            self.yx.hop1()

        def s1b(self):
            for r in (1, -1):
                go(*self.xy.d2[r], *self.yx.d2[r])

        def s2(self):
            self.xy.hop2(0)
            self.yx.hop2(0)
            go(self.sb[0][0])

        def s3(self):
            got(*self.xy.d1h, *self.yx.d1h)
            go(*self.xy.d2[2], *self.yx.d2[2])

        def s4(self):
            got(*self.yx.d2h[0])
            go(self.sb[0][1])

        def s5(self):
            for r in (1, -1):
                self.xy.hop2(r)
                self.yx.hop2(r)
            go(self.sb[1][0], self.sb[-1][0])

        def s6(self):
            self.xy.hop2(2)
            self.yx.hop2(2)

        def s7(self):
            for r in (1, -1):
                got(*self.yx.d2h[r])
                go(self.sb[r][1])

        def s8(self):
            got(*self.xy.d2h[0], *self.xy.d2h[1], *self.xy.d2h[-1])
            go(self.sb[2][0])
            got(*self.xy.d2h[2], *self.yx.d2h[2])
            go(self.sb[2][1])

    TF = FS // 2

    def keep(dd, f):
        if dd in (0, 1):
            return [[acc.at[1, 2 * f + j, (0, 3)[c] if dd == 0 else (1, 2)[c]] for j in range(2)] for c in range(2)]
        if dd == 2:
            return [[zbuf.at[c, 2 * f + j] for j in range(2)] for c in range(2)]
        return [[dwst.at[c, :, pl.ds(pl.multiple_of(f * TF + j * Q, Q), Q)] for j in range(2)] for c in range(2)]

    def forward_h(dd):
        o = IX[dd] * BLK

        def step(f, _):
            fo = pl.multiple_of(f * TF, TF)
            a = _dot(xn[o:o + BLK, :], w1[:, pl.ds(fo, TF)], 1, 0)
            hv, gv = _gelu_and_grad(a)
            h[o:o + BLK, pl.ds(fo, TF)] = hv.astype(BF16)
            for c, row in enumerate(keep(dd, f)):
                for j, ref in enumerate(row):
                    ref[...] = gv[c * OWN:(c + 1) * OWN, j * Q:(j + 1) * Q].reshape(ref.shape)
            return 0

        lax.fori_loop(0, FS // TF, step, 0)

    def backward_h(dd):
        o = IX[dd] * BLK

        def step(f, _):
            fo = pl.multiple_of(f * TF, TF)
            dh = _dot(dy[o:o + BLK, :], w2[pl.ds(fo, TF), :], 1, 1)
            for c, row in enumerate(keep(dd, f)):
                for j, ref in enumerate(row):
                    co = pl.multiple_of(fo + j * Q, Q)
                    da[o + c * OWN:o + (c + 1) * OWN, pl.ds(co, Q)] = (
                        ref[...].reshape(OWN, Q) * dh[c * OWN:(c + 1) * OWN, j * Q:(j + 1) * Q]).astype(BF16)
            return 0

        lax.fori_loop(0, FS // TF, step, 0)

    ROUND = ((0, 0), (1, 0), (1, 1), (0, 1))
    live = {}
    slots = [None, None]
    count = [0]

    def mblk(k, i):
        s, slot, o = k % 2, count[0] % 2, i * BLK
        back, half = ROUND[k]
        count[0] += 1
        if slots[slot] is not None:
            slots[slot].wait_send()

        def step(n, _):
            co = pl.multiple_of(half * C + n * (2 * Q), 2 * Q)
            if back:
                t = _dot(da[o:o + BLK, :], w1[pl.ds(co, 2 * Q), :], 1, 1)
            else:
                t = _dot(h[o:o + BLK, :], w2[:, pl.ds(co, 2 * Q)], 1, 0)
            for j in range(2):
                acc[s, 2 * n + j, i] = t[:OWN, j * Q:(j + 1) * Q].reshape(SIDE, R, Q)
                stage[slot, 2 * n + j] = t[OWN:, j * Q:(j + 1) * Q].reshape(SIDE, R, Q)
            return 0

        lax.fori_loop(0, 2, step, 0)
        if k > 0:
            pl.semaphore_wait(csib.at[i], 1)
        c = remote(stage.at[slot], sibr.at[i], sbs.at[slot], sbr.at[i], sib)
        c.start()
        slots[slot] = c
        live["sib", k, i] = c

    def add(k, i):
        live.pop(("sib", k, i)).wait_recv()
        for q in range(4):
            acc[k % 2, q, i] = acc[k % 2, q, i] + sibr[i, q]
        if k < 3:
            pl.semaphore_signal(csib.at[i], inc=1, device_id=sib, device_id_type=MESH)

    YR, XR = (yp, ym), (xp, xm)

    def ring_copies(get, buf, ss, rs, ring, cut=0, early=False):
        plus, minus = ring
        src = [(get(0, 2), plus), (get(1, 2), minus), (get(1, 1), plus), (get(0, -1), minus), (get(0, 1), plus), (get(1, -1), minus)]
        out = [[remote(v, buf.at[j], ss, rs.at[j], d)] for j, (v, d) in enumerate(src[:6 - 2 * cut])]
        if early:
            for j in range(4):
                v, d = src[j]
                out[j] = [remote(v.at[pl.ds(o, n)], buf.at[j, pl.ds(o, n)], ss, rs.at[j + 8 * c], d)
                          for c, (o, n) in enumerate(((0, 3), (3, 1)))]
        for j in range(6 - 2 * cut, 6):
            v, d = src[j]
            out.append([remote(v.at[pl.ds(o, 2)], buf.at[j, pl.ds(o, 2)], ss, rs.at[j + 2 * c], d)
                        for c, o in enumerate((2, 0))])
        return out

    def p1_get(k, ab):
        if ab == 0:
            return lambda p, r: acc.at[k % 2, p, IX[r]]
        return lambda p, r: acc.at[k % 2, 2 + p, :, IX[r]]

    def p2_get(k, ab):
        return lambda p, r: zbuf.at[k % 2, 2 * ab + p, IX[r]]

    def begin(k):
        if k >= 2:
            for i in range(4):
                pl.semaphore_wait(c1.at[i], 1)
        s = k % 2
        live["c1", k] = [ring_copies(p1_get(k, ab), r1.at[s, ab], p1s.at[s], p1r.at[s, ab], (YR, XR)[ab], k // 3, ab == 1 and k < 2) for ab in range(2)]

    def send_p1(k, js):
        for j in js:
            for ab in range(2):
                for c in live["c1", k][ab][j]:
                    c.start()

    def e1(k):
        begin(k)
        send_p1(k, range(4))

    def e1_early(k):
        begin(k)
        a, b = live["c1", k]
        for j in range(4):
            b[j][0].start()
        for j in (2, 3):
            a[j][0].start()

    def e1_late(k):
        a, b = live["c1", k]
        for j in (0, 1):
            a[j][0].start()
        for j in range(4):
            b[j][1].start()

    def forward(get, buf, cs, ab):
        for j, p, r in ((0, 0, 1), (1, 1, -1)):
            got(*cs[ab][j])
            v = get(p, r)
            v[...] = v[...] + buf[ab, j]
            for c in cs[ab][4 + j]:
                c.start()

    def final(get, buf, cs, ab):
        for j in (2, 3, 4, 5):
            got(*cs[ab][j])
        return (get(0, 0)[...] + buf[ab, 3] + buf[ab, 4], get(1, 0)[...] + buf[ab, 2] + buf[ab, 5])

    def credit(c):
        for i, d in enumerate((ym, yp, xm, xp)):
            pl.semaphore_signal(c.at[i], inc=1, device_id=d, device_id_type=MESH)

    def drained(key):
        live.pop(key)
        buf, ss = {"c1": (r1, p1s), "c2": (r2, p2s)}[key[0]]
        s = key[1] % 2
        pltpu.make_async_copy(buf.at[s], buf.at[s], ss.at[s]).wait()

    def e2(k, abs_=(0, 1)):
        for ab in abs_:
            forward(p1_get(k, ab), r1.at[k % 2], live["c1", k], ab)

    def e3(k):
        s = k % 2
        if k >= 2:
            drained(("c2", k - 2))
            for i in range(4):
                pl.semaphore_wait(c2.at[i], 1)
        ds = [ring_copies(p2_get(k, ab), r2.at[s, ab], p2s.at[s], p2r.at[s, ab], (XR, YR)[ab]) for ab in range(2)]
        live["c2", k] = ds
        for ab in range(2):
            a, b = final(p1_get(k, ab), r1.at[s], live["c1", k], ab)
            zbuf[s, 2 * ab] = a
            zbuf[s, 2 * ab + 1] = b
            for j in range(4):
                ds[ab][j][0].start()
        if k < 2:
            credit(c1)

    def e3_last(k, c):
        s = k % 2
        if c == 0:
            drained(("c2", k - 2))
            for i in range(4):
                pl.semaphore_wait(c2.at[i], 1)
            live["c2", k] = [ring_copies(p2_get(k, ab), r2.at[s, ab], p2s.at[s], p2r.at[s, ab], (XR, YR)[ab]) for ab in range(2)]
        for ab in range(2):
            cs, get, o = live["c1", k][ab], p1_get(k, ab), pl.ds(2 - 2 * c, 2)
            if c == 0:
                got(*cs[2], *cs[3])
            for p, ja, jb in ((0, 3, 4), (1, 2, 5)):
                got(cs[jb][c])
                zbuf[s, 2 * ab + p, o] = get(p, 0)[o] + r1[s, ab, ja, o] + r1[s, ab, jb, o]
            for j in ((0, 1, 3), (2,))[c]:
                live["c2", k][ab][j][0].start()

    def e4(k):
        for ab in range(2):
            forward(p2_get(k, ab), r2.at[k % 2], live["c2", k], ab)

    def e5(k):
        back, half = ROUND[k]
        for ab in range(2):
            a, b = final(p2_get(k, ab), r2.at[k % 2], live["c2", k], ab)
            o = half * C + 2 * ab * Q
            ysum[back, :, o:o + Q] = a
            ysum[back, :, o + Q:o + 2 * Q] = b
        if k < 2:
            credit(c2)

    TM = dwst.shape[1]
    NT2 = FS // TM * (D // FS)
    NT1 = D // TM

    def dw2_copy(i):
        r = pl.multiple_of((i // 2) * TM, TM)
        c = pl.multiple_of((i % 2) * FS, FS)
        return pltpu.make_async_copy(dwst.at[i % 2], dw2_hbm.at[pl.ds(r, TM), pl.ds(c, FS)], lsem.at[3 + i % 2])

    def dw2_tile(i):
        r = pl.multiple_of((i // 2) * TM, TM)
        c = pl.multiple_of((i % 2) * FS, FS)
        return _dot(h[:, pl.ds(r, TM)], dy[:, pl.ds(c, FS)], 0, 0)

    def dw1_tile(i):
        r = pl.multiple_of(i * TM, TM)
        return _dot(xn[:, pl.ds(r, TM)], da[...], 0, 0)

    done = [0]

    def dw(n):
        i0 = done[0]
        done[0] += n
        lo, total = (i0, NT2) if i0 < NT2 else (i0 - NT2, NT1)
        hi = lo + n
        assert hi <= total

        def step2(i, _):
            @pl.when(i >= 2)
            def _():
                dw2_copy(i - 2).wait()
            dwst[i % 2] = dw2_tile(i)
            if lo < NT2 - 2:
                dw2_copy(i).start()
            return 0

        def step1(i, _):
            t = dw1_tile(i)
            for q in range(4):
                v = t[:, q * Q:(q + 1) * Q].reshape(SIDE, R, Q)
                if hi <= SIDE:
                    sibr[i, q] = v
                else:
                    acc[0, q, i - SIDE] = v
            return 0

        lax.fori_loop(lo, hi, step2 if i0 < NT2 else step1, 0)

    gx = Gather(xn, 0)
    gy = Gather(dy, 48)

    gx.s0()
    gx.s1()
    gx.s2()
    gx.s1b()
    gx.s3()
    gx.s4()
    cw1.wait()
    got(*gx.sb[0])
    forward_h(0)
    gx.s5()
    cw2.wait()
    mblk(0, 0)
    gx.s6()
    cdy.wait()
    gy.s0()
    gx.s7()
    gx.s8()
    add(0, 0)
    got(*gx.sb[1])
    forward_h(1)
    gy.s1()
    gy.s2()
    gy.s1b()
    mblk(0, 1)
    got(*gx.sb[-1])
    forward_h(-1)
    gy.s3()
    mblk(0, 2)
    add(0, 1)
    gy.s4()
    got(*gx.sb[2])
    forward_h(2)
    gy.s5()
    add(0, 2)
    e1_early(0)
    mblk(0, 3)
    gy.s6()
    got(*gy.sb[0])
    backward_h(0)
    add(0, 3)
    e1_late(0)
    mblk(1, 0)
    gy.s7()
    got(*gy.sb[1])
    backward_h(1)
    add(1, 0)
    mblk(1, 1)
    gy.s8()
    got(*gy.sb[-1])
    backward_h(-1)
    add(1, 1)
    e2(0)
    mblk(1, 2)
    got(*gy.sb[2])
    backward_h(2)
    add(1, 2)
    mblk(1, 3)
    e1_early(1)
    dw(2)
    add(1, 3)
    e1_late(1)
    e3(0)
    drained(("c1", 0))
    mblk(2, 0)
    mblk(2, 1)
    add(2, 0)
    mblk(2, 2)
    add(2, 1)
    mblk(2, 3)
    add(2, 2)
    e2(1)
    dw(2)
    add(2, 3)
    e1(2)
    e4(0)
    dw(2)
    e3(1)
    drained(("c1", 1))
    mblk(3, 0)
    mblk(3, 1)
    add(3, 0)
    mblk(3, 2)
    add(3, 1)
    mblk(3, 3)
    add(3, 2)
    dw(2)
    add(3, 3)
    e2(2)
    e4(1)
    begin(3)
    send_p1(3, (0, 1))
    e5(0)
    dw(4)
    e3(2)
    send_p1(3, (2, 3))
    drained(("c1", 2))
    dw(2)
    e5(1)
    e4(2)
    e2(3)
    dw(2)
    for i, buf in enumerate((xn, dy)):
        all_sent = buf.at[pl.ds(0, 31 * R)]
        pltpu.make_async_copy(all_sent, all_sent, ags.at[i]).wait()
    pending.clear()

    xhat, rstd = _ln(x_ref[...].astype(F32))
    e5(2)
    dxn = ysum[1]
    gam[0] = jnp.sum(dxn * xhat, axis=0, keepdims=True)
    cs = [remote(gam.at[0], gin.at[0], gs.at[0], gr.at[0], sib)]
    cs += [remote(gam.at[1], gin.at[1 + j], gs.at[1 + j], gr.at[1 + j], d) for j, d in enumerate((xp, xm, xf))]
    cs += [remote(gam.at[2], gin.at[4 + j], gs.at[4 + j], gr.at[4 + j], d) for j, d in enumerate((yp, ym, yf))]
    go(cs[0])
    dxhat = dxn * g_ref[...]
    dx = rstd * (dxhat - jnp.mean(dxhat, axis=-1, keepdims=True) - xhat * jnp.mean(dxhat * xhat, axis=-1, keepdims=True))
    dx_out[...] = (dy[0:R, :].astype(F32) + dx).astype(BF16)
    got(cs[0])
    gam[1] = gam[0] + gin[0]
    go(*cs[1:4])
    e3_last(3, 0)
    e3_last(3, 1)
    got(*cs[1:4])
    gam[2] = gam[1] + gin[1] + gin[2] + gin[3]
    go(*cs[4:7])
    e4(3)
    e5(3)
    y_out[...] = (x_ref[...].astype(F32) + ysum[0]).astype(BF16)
    got(*cs[4:7])
    dg_out[...] = gam[2] + gin[4] + gin[5] + gin[6]
    for c in pending + [v for v in slots]:
        c.wait_send()
    for key in (("c1", 3), ("c2", 2), ("c2", 3)):
        drained(key)


def _out_kernel(y, dx, dg, acc, sibr, dwst, dw2, y_out, dx_out, dg_out, dw1_out, dw2_out, by, bdx, bdg, bdw2, sem, one):
    _, P4, _, S4, R, Q = acc.shape
    keep = dw2.shape[0] - dwst.shape[1]
    reads, writes = [], []
    for s, d, b in ((dw2.at[pl.ds(0, keep)], dw2_out, bdw2), (y, y_out, by), (dx, dx_out, bdx), (dg, dg_out, bdg)):
        m = max(1, s.shape[0] * s.shape[1] * s.dtype.itemsize // 2 ** 20)
        r = s.shape[0] // m
        for i in range(m):
            j = len(reads)
            part = pl.ds(i * r, r)
            reads.append(pltpu.make_async_copy(s.at[part], b.at[part], sem.at[0, j]))
            writes.append(pltpu.make_async_copy(b.at[part], d.at[part], sem.at[1, j]))
    for c in reads:
        c.start()
    W = dwst.shape[2]
    tail = [pltpu.make_async_copy(dwst.at[c], dw2_out.at[pl.ds(keep, dwst.shape[1]), pl.ds(c * W, W)], one.at[1 + c]) for c in range(2)]
    for c in tail:
        c.start()
    for t in range(2 * S4):
        for q in range(P4):
            src = sibr.at[t, q] if t < S4 else acc.at[0, q, t - S4]
            pltpu.make_async_copy(src, dw1_out.at[pl.ds(t * S4, S4), :, pl.ds(q * Q, Q)], one.at[0]).start()
    for c, w in zip(reads, writes):
        c.wait()
        w.start()
    for w in writes + tail:
        w.wait()
    pltpu.make_async_copy(dw1_out, dw1_out, one.at[0]).wait()


def solution(mesh):
    rows = P(("data", "tp"), None)
    assert mesh.shape["tp"] == 2 * SIDE * SIDE

    def body(X, gamma, W1, W2, dY):
        R, D = X.shape
        FS = W1.shape[1]
        T = R * 2 * SIDE * SIDE
        C = D // 2
        Q = C // 4
        vm = pl.BlockSpec(memory_space=pltpu.VMEM)
        anyspace = pl.BlockSpec(memory_space=pl.ANY)
        dma = pltpu.SemaphoreType.DMA
        reg = pltpu.SemaphoreType.REGULAR
        raw = pl.pallas_call(
            _kernel,
            out_shape=(
                jax.ShapeDtypeStruct((R, D), BF16),
                jax.ShapeDtypeStruct((R, D), BF16),
                jax.ShapeDtypeStruct((1, D), F32),
                pltpu.VMEM((2, 4, SIDE, SIDE, R, Q), F32),
                pltpu.VMEM((SIDE, 4, SIDE, R, Q), F32),
                pltpu.VMEM((2, 256, FS), F32),
                jax.ShapeDtypeStruct((FS, D), F32),
            ),
            in_specs=[vm, vm, anyspace, anyspace, anyspace],
            out_specs=(vm, vm, vm, vm, vm, vm, anyspace),
            scratch_shapes=[
                pltpu.VMEM((T, D), BF16),
                pltpu.VMEM((T, D), BF16),
                pltpu.VMEM((T, FS), BF16),
                pltpu.VMEM((T, FS), BF16),
                pltpu.VMEM((D, FS), BF16),
                pltpu.VMEM((FS, D), BF16),
                pltpu.VMEM((2, 4, SIDE, R, Q), F32),
                pltpu.VMEM((2, 4, SIDE, R, Q), F32),
                pltpu.VMEM((2, 2, 6, SIDE, R, Q), F32),
                pltpu.VMEM((2, 2, 6, R, Q), F32),
                pltpu.VMEM((2, R, D), F32),
                pltpu.VMEM((3, 1, D), F32),
                pltpu.VMEM((7, 1, D), F32),
                dma((2,)), dma((96,)),
                dma((2,)), dma((2, 2, 12)),
                dma((2,)), dma((2, 2, 6)),
                dma((2,)), dma((SIDE,)),
                dma((7,)), dma((7,)),
                dma((5,)),
                reg((4,)), reg((4,)), reg((SIDE,)),
            ],
            compiler_params=pltpu.CompilerParams(
                collective_id=0, has_side_effects=True, vmem_limit_bytes=67043328 - 14 * 2 ** 20 - 2 ** 17),
        )(X, gamma.reshape(1, D), W1, W2, dY)
        Y, dX, dg, acc, sibr, dwst, dW2 = raw
        dwst = pltpu.with_memory_space_constraint(dwst, pltpu.VMEM)
        acc = pltpu.with_memory_space_constraint(acc, pltpu.VMEM)
        sibr = pltpu.with_memory_space_constraint(sibr, pltpu.VMEM)
        Y, dX, dg, dW2 = (pltpu.with_memory_space_constraint(v, pltpu.HBM) for v in (Y, dX, dg, dW2))
        Y, dX, dg, dW1, dW2 = pl.pallas_call(
            _out_kernel,
            out_shape=(
                jax.ShapeDtypeStruct((R, D), BF16),
                jax.ShapeDtypeStruct((R, D), BF16),
                jax.ShapeDtypeStruct((1, D), F32),
                jax.ShapeDtypeStruct((D // R, R, FS), F32),
                jax.ShapeDtypeStruct((FS, D), F32),
            ),
            in_specs=[anyspace, anyspace, anyspace, vm, vm, vm, anyspace],
            out_specs=(anyspace,) * 5,
            scratch_shapes=[pltpu.VMEM((R, D), BF16), pltpu.VMEM((R, D), BF16), pltpu.VMEM((1, D), F32),
                            pltpu.VMEM((FS, D), F32), dma((2, 16)), dma((3,))],
            compiler_params=pltpu.CompilerParams(vmem_limit_bytes=67043328 - 14 * 2 ** 20 - 2 ** 17),
        )(Y, dX, dg, acc, sibr, dwst, dW2)
        return Y, dX, dW1.reshape(D, FS), dW2, dg.reshape(D)

    return jax.shard_map(body, mesh=mesh,
                         in_specs=(rows, P(None), P(None, "tp"), P("tp", None), rows),
                         out_specs=(rows, rows, P("data", "tp"), rows, P("data")),
                         check_vma=False)
```
